128 devices in a mesh: cuts: 8 (over z, x_lo), row: 16 (over x_hi, y, core).
Axes of the slice: x: 4 (x_hi: 2, x_lo: 2; x = x_hi * 2 + x_lo), y: 4, z: 4, core: 2. Of those that a mesh axis runs over, the one named last changes fastest.
Arguments:
- eigvecs: float32 [16384, 4096], P('row', 'cuts'), may hold values from -1.2 to 1.2
- slice_counts: int32 [8], P('cuts'), may hold values from 256 to 512, as said below
- occ_index: int32 [4096], P('cuts'), may hold values from 0 to 63
- occ_levels: float32 [64], replicated, may hold values from 0 to 1
Outputs:
- slab: float32 [4096, 16384], P('cuts', 'row')
The draws below stay inside these ranges and needn't reach their ends.
Inputs may be any that keep to these rules, and one draw needn't show every extreme that they name: `slice_counts`: some slice holds exactly 512 eigenvalues in every draw; the others at least half of that.
All inputs are finite; a program needn't handle non-finite values.
Results may differ from the reference program's by a relative error of at most 0.000062.
Values sent between devices are 32-bit elements; how exact they have to be, the bound alone decides.
A program may use at most 128 MiB of HBM per device.

```python
import jax
import jax.numpy as jnp
from jax import lax

ORDER = 16384
BLOCK = 1024
SLAB_SUB = 256
EIG_DEV = 512
LEVELS = 64
EIGS = 4096
SLAB = 4096
N_CUTS = 8


def draw_slice_counts(key, part):
    first, second = jax.random.split(jax.random.fold_in(key, 11))
    counted = jax.random.randint(first, (N_CUTS,), EIG_DEV // 2, EIG_DEV + 1)
    full_one = jax.random.randint(second, (), 0, N_CUTS)
    return jnp.where(jnp.arange(N_CUTS) == full_one, EIG_DEV, counted).astype(jnp.int32)


def with_ends(array, stream_key, low, top_value):
    longest = array.shape.index(max(array.shape))
    spots = []
    for shift in (0, 1):
        where = [jax.random.randint(jax.random.fold_in(stream_key, axis), (), 0, length) for axis, length in enumerate(array.shape)]
        where[longest] = (where[longest] + shift) % array.shape[longest]
        spots.append(tuple(where))
    return array.at[spots[0]].set(low).at[spots[1]].set(top_value)


def block_levels(key, dims, pieces, low, largest):
    factor_of, own = 1.0, jax.random.fold_in(key, 6)
    for position, shards_of in pieces:
        draws = jnp.exp(jax.random.uniform(jax.random.fold_in(own, position), (shards_of,), jnp.float32, low / len(pieces), largest / len(pieces)))
        factor_of = factor_of * jnp.repeat(draws, dims[position] // shards_of).reshape([-1 if axis == position else 1 for axis in range(len(dims))])
    return factor_of


def gaussian(own_key, shape, width, reach, pieces=(), held_as=jnp.bfloat16):
    array = jax.random.normal(own_key, shape, jnp.float32) * width
    if len(pieces) > 0:
        array = block_levels(own_key, shape, pieces, -0.22, 0.18) * array
    return jnp.clip(array, min=-reach, max=reach).astype(held_as)


def setup_inputs(seed: int = 0) -> dict:
    key_of = jax.random.split(jax.random.key(seed), 5)
    eigvecs = gaussian(key_of[0], (ORDER, EIGS), 0.18, 1.2, ((0, 16), (1, 8)), jnp.float32)
    slice_counts = draw_slice_counts(jax.random.fold_in(key_of[4], 71), 0)
    occ_index = with_ends(jax.random.randint(key_of[2], (EIGS,), 0, LEVELS), jax.random.fold_in(key_of[2], 1), 0, LEVELS - 1).astype(jnp.int32)
    occ_levels = jnp.clip(jax.random.uniform(key_of[3], (LEVELS,), jnp.float32, 0.0, 1.0), 0.0, 1.0)
    return dict(eigvecs=eigvecs, slice_counts=slice_counts, occ_index=occ_index, occ_levels=occ_levels)


def reference(eigvecs, slice_counts, occ_index, occ_levels):
    slots = jnp.arange(EIGS, dtype=jnp.int32)
    group = slots // EIG_DEV
    inside = slots - group * EIG_DEV
    live = inside < slice_counts[group]
    weights = jnp.where(live, occ_levels[occ_index], jnp.float32(0.0))
    blocks = eigvecs.reshape(ORDER // BLOCK, BLOCK, EIGS)[:, :SLAB_SUB, :]
    picked = blocks.reshape(SLAB, EIGS) * weights[None, :]
    return lax.dot_general(picked, eigvecs, (((1,), (1,)), ((), ())), precision=lax.Precision.HIGHEST, preferred_element_type=jnp.float32)
```

```python
import jax
import jax.numpy as jnp
from jax import lax
from jax.experimental import pallas as pl
from jax.experimental.pallas import tpu as pltpu
from jax.sharding import PartitionSpec as P

MESH = pl.DeviceIdType.MESH
SUB = 256
HALVES = 2
HROWS = SUB // HALVES
CHUNKS = 4
F32, BF16 = jnp.float32, jnp.bfloat16


def split(value):
    high = value.astype(BF16)
    return high, (value - high.astype(F32)).astype(BF16)


def kernel(
    e_ref, idx_ref, lev_ref, cnt_ref, out_ref,
    p_buf, own_p, e_in, p_hi, p_lo, e_hi, e_lo, part, zin,
    xs_sem, ys_sem, cs_sem, p_sem, es_sem, er_sem, as_sem, ar_sem, zs_sem, zr_sem,
):
    rows, depth = e_ref.shape
    width = rows // CHUNKS
    c, r = lax.axis_index("cuts"), lax.axis_index("row")
    z, xl = c // 2, lax.rem(c, 2)
    q, core = r // 2, lax.rem(r, 2)
    xh, y = q // 4, lax.rem(q, 4)
    x = xh * 2 + xl

    def device(dx=0, dy=0, dz=0, dcore=0):
        nx, ny = lax.rem(x + dx + 4, 4), lax.rem(y + dy + 4, 4)
        nz, ncore = lax.rem(z + dz + 4, 4), lax.rem(core + dcore, 2)
        return (nz * 2 + lax.rem(nx, 2), ((nx // 2) * 4 + ny) * 2 + ncore)

    pair = (z * 2 + 1 - xl, r)
    source = lax.rem(y, 2) == xl
    own_rel = lax.rem(2 * xh + y // 2 - z + 4, 4)
    even_row = y // 2 == lax.rem(z, 2)

    def row_gap(rel):
        return lax.rem(2 * lax.rem(z + rel, 2) + xl - y + 4, 4)

    barrier = pltpu.get_barrier_semaphore()
    for peer in (
        device(dx=1), device(dx=2), device(dx=3), device(dy=1), device(dy=3),
        device(dz=1), device(dz=3), device(dcore=1),
    ):
        pl.semaphore_signal(barrier, inc=1, device_id=peer, device_id_type=MESH)

    level = lax.broadcasted_iota(jnp.int32, (lev_ref.shape[0], depth), 0)
    chosen = jnp.where(level == idx_ref[...], lev_ref[...], F32(0.0))
    values = jnp.sum(chosen, axis=0, keepdims=True)
    live = lax.broadcasted_iota(jnp.int32, (1, depth), 1) < cnt_ref[0]
    weights = jnp.where(live, values, F32(0.0))
    for h in range(HALVES):
        own_p[h] = e_ref[h * HROWS : (h + 1) * HROWS, :] * weights

    @pl.when(source)
    def _():
        for h in range(HALVES):
            p_buf[own_rel, core, 0, h] = own_p[h]

    pl.semaphore_wait(barrier, 8)

    def copy(src, dst, send, recv, peer):
        return pltpu.make_async_remote_copy(
            src_ref=src, dst_ref=dst, send_sem=send, recv_sem=recv,
            device_id=peer, device_id_type=MESH,
        )

    def x_copy(h, side, s, peer):
        slot = p_buf.at[own_rel, core, s, h]
        return copy(own_p.at[h], slot, xs_sem.at[side, h], p_sem.at[own_rel, core, s, h], peer)

    def y_copy(rel, s, h, up):
        slot = p_buf.at[rel, core, s, h]
        side = 0 if up else 1
        return copy(
            slot, slot, ys_sem.at[side, rel, s, h], p_sem.at[rel, core, s, h],
            device(dy=1 if up else 3),
        )

    def core_copy(rel, s, h):
        slot = p_buf.at[rel, core, s, h]
        return copy(slot, slot, cs_sem.at[rel, s, h], p_sem.at[rel, core, s, h], device(dcore=1))

    def e_copy(j):
        return copy(
            e_ref.at[pl.ds(j * width, width)], e_in.at[j], es_sem.at[j], er_sem.at[j], pair
        )

    for h in range(HALVES):
        @pl.when(source)
        def _():
            x_copy(h, 0, 0, device(dx=2)).start()

        @pl.when(jnp.logical_not(source))
        def _():
            x_copy(h, 0, 1, device(dx=1)).start()
            x_copy(h, 1, 1, device(dx=3)).start()
    for j in range(CHUNKS):
        e_copy(j).start()

    for j in range(CHUNKS):
        span = pl.ds(j * width, width)
        high, low = split(e_ref[span, :])
        e_hi[span, :depth] = high
        e_lo[span, :depth] = low

    def arrive(rel, k, s, h):
        slot = p_buf.at[rel, k, s, h]
        pltpu.make_async_copy(slot, slot, p_sem.at[rel, k, s, h]).wait()

    def keep(rel, k, s, h):
        high, low = split(p_buf[rel, k, s, h])
        rows_of = pl.ds(h * HROWS, HROWS)
        p_hi[rel, k, rows_of, s * depth : (s + 1) * depth] = high
        p_lo[rel, k, rows_of, s * depth : (s + 1) * depth] = low

    def sends_up(rel, s):
        gap = row_gap(rel)
        return (gap == 0) | (gap == 3) if s == 0 else gap == 0

    def sends_down(rel, s):
        gap = row_gap(rel)
        return (gap == 0) | (gap == 1) if s == 1 else gap == 0

    def relay(rel, s, h):
        mine = source & (rel == own_rel) if s == 0 else None

        def take():
            arrive(rel, core, s, h)

        if mine is None:
            take()
        else:
            pl.when(jnp.logical_not(mine))(take)

        @pl.when(sends_up(rel, s))
        def _():
            y_copy(rel, s, h, True).start()

        @pl.when(sends_down(rel, s))
        def _():
            y_copy(rel, s, h, False).start()

        core_copy(rel, s, h).start()
        keep(rel, core, s, h)

    @pl.when(source)
    def _():
        for even, odd in (((2, 0), (1, 0)), ((2, 1), (3, 0)), ((0, 0), (1, 1)), ((0, 1), (3, 1))):
            rel = jnp.where(even_row, even[0], odd[0])
            h = jnp.where(even_row, even[1], odd[1])
            for s in range(2):
                relay(rel, s, h)

    def get_block(rel, h):
        @pl.when(jnp.logical_not(source & (row_gap(rel) == 0)))
        def _():
            for s in range(2):
                relay(rel, s, h)

        for s in range(2):
            arrive(rel, 1 - core, s, h)
            keep(rel, 1 - core, s, h)

    def get_rows(j):
        e_copy(j).wait_recv()
        span = pl.ds(j * width, width)
        high, low = split(e_in[j])
        e_hi[span, depth:] = high
        e_lo[span, depth:] = low

    def dot(a, b):
        return lax.dot_general(a, b, (((1,), (1,)), ((), ())), preferred_element_type=F32)

    def tile(rel, k, rows_of, j):
        span = pl.ds(j * width, width)
        high, low = p_hi[rel, k, rows_of, :], p_lo[rel, k, rows_of, :]
        e_high, e_low = e_hi[span, :], e_lo[span, :]
        return dot(high, e_high) + (dot(high, e_low) + dot(low, e_high))

    def ring(way):
        nz = lax.rem(z + 1 + 2 * way, 4)
        return (nz * 2 + xl, r)

    def first_copy(way, h, j):
        rows_of = pl.ds(h * HROWS, HROWS)
        return copy(
            part.at[0, way, j, rows_of], zin.at[0, way, j, rows_of],
            as_sem.at[way, h, j], ar_sem.at[way, h, j], ring(way),
        )

    def later_copy(kind, way, j):
        return copy(
            part.at[kind, way, j], zin.at[kind, way, j],
            zs_sem.at[kind - 1, way, j], zr_sem.at[kind - 1, way, j], ring(way),
        )

    def first(h, j):
        def body(way, carry):
            rows_of = pl.ds(h * HROWS, HROWS)
            part[0, way, j, rows_of] = tile(2, way, rows_of, j)
            first_copy(way, h, j).start()
            return carry

        lax.fori_loop(0, 2, body, 0)

    def second(j):
        def body(way, carry):
            part[1, way, j] = tile(1 + 2 * way, 1 - way, pl.ds(0, SUB), j)
            later_copy(1, way, j).start()
            return carry

        lax.fori_loop(0, 2, body, 0)

    def third(j):
        def body(way, carry):
            total = tile(1 + 2 * way, way, pl.ds(0, SUB), j)
            for h in range(HALVES):
                first_copy(way, h, j).wait_recv()
            part[2, way, j] = total + zin[0, way, j]
            later_copy(2, way, j).start()
            return carry

        lax.fori_loop(0, 2, body, 0)

    def last(j):
        def body(k, carry):
            rows_of = pl.ds(k * SUB, SUB)
            out_ref[rows_of, j * width : (j + 1) * width] = tile(0, k, pl.ds(0, SUB), j)
            return carry

        lax.fori_loop(0, 2, body, 0)

    def finish(j):
        def body(k, carry):
            rows_of = pl.ds(k * SUB, SUB)
            later_copy(1, 1 - k, j).wait_recv()
            later_copy(2, k, j).wait_recv()
            out_ref[rows_of, j * width : (j + 1) * width] += zin[2, k, j] + zin[1, 1 - k, j]
            return carry

        lax.fori_loop(0, 2, body, 0)

    get_block(2, 0)
    get_rows(0)
    first(0, 0)
    get_block(2, 1)
    first(1, 0)
    get_rows(1)
    first(0, 1)
    first(1, 1)
    get_block(1, 0)
    get_block(3, 0)
    get_block(1, 1)
    get_block(3, 1)
    second(0)
    third(0)
    get_block(0, 0)
    get_block(0, 1)
    second(1)
    third(1)
    get_rows(2)
    first(0, 2)
    first(1, 2)
    second(2)
    third(2)
    get_rows(3)
    first(0, 3)
    first(1, 3)
    second(3)
    third(3)
    for j in range(CHUNKS):
        last(j)
    for j in range(CHUNKS):
        finish(j)

    for h in range(HALVES):
        @pl.when(source)
        def _():
            x_copy(h, 0, 0, device(dx=2)).wait_send()

        @pl.when(jnp.logical_not(source))
        def _():
            x_copy(h, 0, 1, device(dx=1)).wait_send()
            x_copy(h, 1, 1, device(dx=3)).wait_send()
    for j in range(CHUNKS):
        e_copy(j).wait_send()
    for rel in range(4):
        for s in range(2):
            for h in range(HALVES):
                @pl.when(sends_up(rel, s))
                def _():
                    y_copy(rel, s, h, True).wait_send()

                @pl.when(sends_down(rel, s))
                def _():
                    y_copy(rel, s, h, False).wait_send()

                core_copy(rel, s, h).wait_send()
    for j in range(CHUNKS):
        for way in range(2):
            for h in range(HALVES):
                first_copy(way, h, j).wait_send()
            later_copy(1, way, j).wait_send()
            later_copy(2, way, j).wait_send()


def shards(eigvecs, slice_counts, occ_index, occ_levels):
    rows, depth = eigvecs.shape
    width = rows // CHUNKS
    dma = pltpu.SemaphoreType.DMA
    vmem = pl.BlockSpec(memory_space=pltpu.VMEM)
    return pl.pallas_call(
        kernel,
        out_shape=jax.ShapeDtypeStruct((2 * SUB, rows), F32),
        in_specs=[vmem, vmem, vmem, pl.BlockSpec(memory_space=pltpu.SMEM)],
        out_specs=vmem,
        scratch_shapes=[
            pltpu.VMEM((4, 2, 2, HALVES, HROWS, depth), F32),
            pltpu.VMEM((HALVES, HROWS, depth), F32),
            pltpu.VMEM((CHUNKS, width, depth), F32),
            pltpu.VMEM((4, 2, SUB, 2 * depth), BF16),
            pltpu.VMEM((4, 2, SUB, 2 * depth), BF16),
            pltpu.VMEM((rows, 2 * depth), BF16),
            pltpu.VMEM((rows, 2 * depth), BF16),
            pltpu.VMEM((3, 2, CHUNKS, SUB, width), F32),
            pltpu.VMEM((3, 2, CHUNKS, SUB, width), F32),
            dma((2, HALVES)),
            dma((2, 4, 2, HALVES)),
            dma((4, 2, HALVES)),
            dma((4, 2, 2, HALVES)),
            dma((CHUNKS,)),
            dma((CHUNKS,)),
            dma((2, HALVES, CHUNKS)),
            dma((2, HALVES, CHUNKS)),
            dma((2, 2, CHUNKS)),
            dma((2, 2, CHUNKS)),
        ],
        compiler_params=pltpu.CompilerParams(
            collective_id=0, has_side_effects=True, vmem_limit_bytes=60 * 1024 * 1024
        ),
    )(eigvecs, occ_index.reshape(1, depth), occ_levels.reshape(-1, 1), slice_counts)


def solution(mesh):
    return jax.shard_map(
        shards,
        mesh=mesh,
        in_specs=(P("row", "cuts"), P("cuts"), P("cuts"), P()),
        out_specs=P("cuts", "row"),
        check_vma=False,
    )
```

```python
import jax
import jax.numpy as jnp
from jax import lax
from jax.experimental import pallas as pl
from jax.experimental.pallas import tpu as pltpu
from jax.sharding import PartitionSpec as P

MESH = pl.DeviceIdType.MESH
SUB = 256
HALVES = 2
HROWS = SUB // HALVES
CHUNKS = 4
F32, BF16 = jnp.float32, jnp.bfloat16


def split(value):
    high = value.astype(BF16)
    return high, (value - high.astype(F32)).astype(BF16)


def kernel(
    e_ref, idx_ref, lev_ref, cnt_ref, out_ref,
    p_buf, own_p, via_x, via_y, w_own, w_in, e_in, p_hi, p_lo, e_hi, e_lo, part, zin,
    w_sem, vx_sem, vy_sem, xs_sem, ys_sem, cs_sem, p_sem, es_sem, er_sem, zs_sem, zr_sem,
):
    rows, depth = e_ref.shape
    width = rows // CHUNKS
    c, r = lax.axis_index("cuts"), lax.axis_index("row")
    z, xl = c // 2, lax.rem(c, 2)
    q, core = r // 2, lax.rem(r, 2)
    xh, y = q // 4, lax.rem(q, 4)
    x = xh * 2 + xl

    def device(dx=0, dy=0, dz=0, dcore=0):
        nx, ny = lax.rem(x + dx + 4, 4), lax.rem(y + dy + 4, 4)
        nz, ncore = lax.rem(z + dz + 4, 4), lax.rem(core + dcore, 2)
        return (nz * 2 + lax.rem(nx, 2), ((nx // 2) * 4 + ny) * 2 + ncore)

    pair = (z * 2 + 1 - xl, r)
    other = device(dx=3 - 2 * xl)
    source = lax.rem(y, 2) == xl
    even_row = y // 2 == lax.rem(z, 2)
    bridge = jnp.logical_not(source)
    source_even = source & even_row
    source_odd = source & jnp.logical_not(even_row)

    def base(dy):
        return lax.rem(2 * xh + lax.rem(y + dy, 4) // 2 - z + 4, 4)

    own_rel = base(0)
    far_rel = lax.rem(own_rel + 2, 4)

    def row_gap(rel):
        return lax.rem(2 * lax.rem(z + rel, 2) + xl - y + 4, 4)

    barrier = pltpu.get_barrier_semaphore()
    for peer in (
        device(dx=1), device(dx=3), device(dy=1), device(dy=3),
        device(dz=1), device(dz=3), device(dcore=1),
    ):
        pl.semaphore_signal(barrier, inc=1, device_id=peer, device_id_type=MESH)

    level = lax.broadcasted_iota(jnp.int32, (lev_ref.shape[0], depth), 0)
    chosen = jnp.where(level == idx_ref[...], lev_ref[...], F32(0.0))
    values = jnp.sum(chosen, axis=0, keepdims=True)
    live = lax.broadcasted_iota(jnp.int32, (1, depth), 1) < cnt_ref[0]
    weights = jnp.where(live, values, F32(0.0))
    w_own[...] = jnp.broadcast_to(weights, w_own.shape)
    for h in range(HALVES):
        own_p[h] = e_ref[h * HROWS : (h + 1) * HROWS, :] * weights

    @pl.when(source)
    def _():
        for h in range(HALVES):
            p_buf[own_rel, core, 0, h] = own_p[h]

    pl.semaphore_wait(barrier, 7)

    def copy(src, dst, send, recv, peer):
        return pltpu.make_async_remote_copy(
            src_ref=src, dst_ref=dst, send_sem=send, recv_sem=recv,
            device_id=peer, device_id_type=MESH,
        )

    def w_copy():
        return copy(w_own, w_in, w_sem.at[0], w_sem.at[1], pair)

    def e_copy(i):
        return copy(
            e_ref.at[pl.ds(i * HROWS, HROWS)], e_in.at[i], es_sem.at[i], er_sem.at[i], pair
        )

    def slot_of(rel, s, h):
        return p_buf.at[rel, core, s, h], p_sem.at[rel, core, s, h]

    def to_via_x(h):
        return copy(own_p.at[h], via_x.at[h], xs_sem.at[0, h], vx_sem.at[h], other)

    def from_via_x(h):
        slot, recv = slot_of(far_rel, 0, h)
        return copy(via_x.at[h], slot, xs_sem.at[1, h], recv, pair)

    def to_source(h):
        slot, recv = slot_of(own_rel, 1, h)
        return copy(own_p.at[h], slot, xs_sem.at[0, h], recv, other)

    def to_via_y(side, h):
        return copy(
            own_p.at[h], via_y.at[side, h], xs_sem.at[2 + side, h], vy_sem.at[side, h],
            device(dy=3 if side == 0 else 1),
        )

    def from_via_y(side, h):
        slot, recv = slot_of(base(1 if side == 0 else 3), 1, h)
        return copy(via_y.at[side, h], slot, xs_sem.at[2 + side, h], recv, other)

    def y_copy(rel, s, h, up):
        slot, recv = slot_of(rel, s, h)
        return copy(
            slot, slot, ys_sem.at[0 if up else 1, rel, s, h], recv, device(dy=1 if up else 3)
        )

    def core_copy(rel, s, h):
        slot, recv = slot_of(rel, s, h)
        return copy(slot, slot, cs_sem.at[rel, s, h], recv, device(dcore=1))

    def landed(ref, sem):
        pltpu.make_async_copy(ref, ref, sem).wait()

    def arrive(rel, k, s, h):
        landed(p_buf.at[rel, k, s, h], p_sem.at[rel, k, s, h])

    def keep(rel, k, s, h):
        high, low = split(p_buf[rel, k, s, h])
        rows_of = pl.ds(h * HROWS, HROWS)
        p_hi[rel, k, rows_of, s * depth : (s + 1) * depth] = high
        p_lo[rel, k, rows_of, s * depth : (s + 1) * depth] = low

    def sends(rel, s, up):
        gap = row_gap(rel)
        first_hop = gap == 0
        if s == 1:
            first_hop = first_hop & (rel != far_rel)
        if up and s == 0:
            return first_hop | (gap == 3)
        if not up and s == 1:
            return first_hop | (gap == 1)
        return first_hop

    def hand_on(rel, s, h):
        for up in (True, False):
            pl.when(sends(rel, s, up))(lambda up=up: y_copy(rel, s, h, up).start())
        core_copy(rel, s, h).start()
        keep(rel, core, s, h)

    def take(rel, s, h):
        arrive(rel, core, s, h)
        hand_on(rel, s, h)

    def weigh(h):
        landed(e_in.at[h], er_sem.at[h])
        p_buf[own_rel, core, 1, h] = e_in[h] * w_in[0:1, :]
        hand_on(own_rel, 1, h)

    def need(rel, h):
        for s in range(2):
            arrive(rel, 1 - core, s, h)
            keep(rel, 1 - core, s, h)

    def take_far(h):
        far = base(2)
        far_next = lax.rem(far + 2, 4)
        take(far, 0, h)
        take(far, 1, h)
        take(far_next, 0, h)
        take(far_next, 1, h)

    def take_sides(h):
        up, down = base(1), base(3)
        up_next, down_next = lax.rem(up + 2, 4), lax.rem(down + 2, 4)
        take(up, 0, h)
        take(down, 0, h)
        take(up, 1, h)
        take(down, 1, h)
        take(up_next, 0, h)
        take(down_next, 0, h)
        take(up_next, 1, h)
        take(down_next, 1, h)

    def begin_source():
        to_via_x(0).start()
        w_copy().start()
        for i in range(2 * CHUNKS):
            e_copy(i).start()
        hand_on(own_rel, 0, 0)
        landed(w_in, w_sem.at[1])
        weigh(0)
        for side in range(2):
            landed(via_y.at[side, 0], vy_sem.at[side, 0])
            from_via_y(side, 0).start()
        to_via_x(1).start()
        take(far_rel, 1, 0)
        take(far_rel, 0, 0)
        hand_on(own_rel, 0, 1)
        for side in range(2):
            landed(via_y.at[side, 1], vy_sem.at[side, 1])
            from_via_y(side, 1).start()
        take(far_rel, 1, 1)
        weigh(1)

    def begin_bridge():
        for h in range(HALVES):
            to_source(h).start()
            for side in range(2):
                to_via_y(side, h).start()
        w_copy().start()
        e_copy(0).start()
        landed(w_in, w_sem.at[1])
        landed(via_x.at[0], vx_sem.at[0])
        from_via_x(0).start()
        e_copy(1).start()
        e_copy(2).start()
        take_sides(0)
        landed(via_x.at[1], vx_sem.at[1])
        from_via_x(1).start()
        for i in range(3, 2 * CHUNKS):
            e_copy(i).start()
        for i in range(2):
            landed(e_in.at[i], er_sem.at[i])

    def split_rows(j):
        span = pl.ds(j * width, width)
        high, low = split(e_ref[span, :])
        e_hi[span, :depth] = high
        e_lo[span, :depth] = low

    def get_rows(j):
        for i in range(2):
            if j > 0:
                landed(e_in.at[2 * j + i], er_sem.at[2 * j + i])
            span = pl.ds(j * width + i * HROWS, HROWS)
            high, low = split(e_in[2 * j + i])
            e_hi[span, depth:] = high
            e_lo[span, depth:] = low

    def dot(a, b):
        return lax.dot_general(a, b, (((1,), (1,)), ((), ())), preferred_element_type=F32)

    def tile(rel, k, rows_of, j):
        span = pl.ds(j * width, width)
        high, low = p_hi[rel, k, rows_of, :], p_lo[rel, k, rows_of, :]
        e_high, e_low = e_hi[span, :], e_lo[span, :]
        return dot(high, e_high) + (dot(high, e_low) + dot(low, e_high))

    def z_copy(kind, way, h, j):
        rows_of = pl.ds(h * HROWS, HROWS)
        nz = lax.rem(z + 1 + 2 * way, 4)
        return copy(
            part.at[kind, way, j, rows_of], zin.at[kind, way, j, rows_of],
            zs_sem.at[kind, way, h, j], zr_sem.at[kind, way, h, j], (nz * 2 + xl, r),
        )

    def z_landed(kind, way, h, j):
        landed(zin.at[kind, way, j, pl.ds(h * HROWS, HROWS)], zr_sem.at[kind, way, h, j])

    def stage(kind, halves, j):
        rows_of = pl.ds(halves[0] * HROWS, len(halves) * HROWS)

        def step(way, carry):
            if kind == 0:
                total = tile(2, way, rows_of, j)
            elif kind == 1:
                total = tile(1 + 2 * way, 1 - way, rows_of, j)
            else:
                total = tile(1 + 2 * way, way, rows_of, j)
                for h in halves:
                    z_landed(0, way, h, j)
                total = total + zin[0, way, j, rows_of]
            part[kind, way, j, rows_of] = total
            for h in halves:
                z_copy(kind, way, h, j).start()
            return carry

        lax.fori_loop(0, 2, step, 0)

    def first(halves, j):
        stage(0, halves, j)

    def second(halves, j):
        stage(1, halves, j)

    def third(halves, j):
        stage(2, halves, j)

    def last(j):
        def step(k, carry):
            rows_of = pl.ds(k * SUB, SUB)
            out_ref[rows_of, j * width : (j + 1) * width] = tile(0, k, pl.ds(0, SUB), j)
            return carry

        lax.fori_loop(0, 2, step, 0)

    def finish(j):
        def step(k, carry):
            rows_of = pl.ds(k * SUB, SUB)
            for h in range(HALVES):
                z_landed(1, 1 - k, h, j)
                z_landed(2, k, h, j)
            out_ref[rows_of, j * width : (j + 1) * width] += zin[2, k, j] + zin[1, 1 - k, j]
            return carry

        lax.fori_loop(0, 2, step, 0)

    def begin():
        pl.when(source)(begin_source)
        pl.when(bridge)(begin_bridge)

    def some_first():
        @pl.when(source_even)
        def _():
            need(2, 0)
            first((0,), 0)

        @pl.when(source_odd)
        def _():
            need(1, 0)
            need(3, 0)
            second((0,), 0)

    def other_first():
        @pl.when(source)
        def _():
            take_far(0)

        @pl.when(jnp.logical_not(source_even))
        def _():
            need(2, 0)
            first((0,), 0)

        @pl.when(jnp.logical_not(source_odd))
        def _():
            need(1, 0)
            need(3, 0)
            second((0,), 0)

    def row_rest():
        @pl.when(source)
        def _():
            take(far_rel, 0, 1)

    def side_rest():
        pl.when(source)(lambda: take_far(1))
        pl.when(bridge)(lambda: take_sides(1))
        for rel in (2, 1, 3):
            need(rel, 1)

    for j in range(CHUNKS):
        split_rows(j)
    begin()
    get_rows(0)
    some_first()
    other_first()
    row_rest()
    third((0,), 0)
    get_rows(1)
    first((0,), 1)
    second((0,), 1)
    third((0,), 1)
    side_rest()
    first((1,), 0)
    second((1,), 0)
    third((1,), 0)
    first((1,), 1)
    second((1,), 1)
    third((1,), 1)
    get_rows(2)
    first((0, 1), 2)
    second((0, 1), 2)
    third((0, 1), 2)
    get_rows(3)
    first((0, 1), 3)
    second((0, 1), 3)
    third((0, 1), 3)
    need(0, 0)
    need(0, 1)
    for j in range(CHUNKS):
        last(j)
    for j in range(CHUNKS):
        finish(j)

    w_copy().wait_send()
    for i in range(2 * CHUNKS):
        e_copy(i).wait_send()
    for h in range(HALVES):
        for lane in range(4):
            if lane == 1:
                pl.when(bridge)(lambda: from_via_x(h).wait_send())
            elif lane == 0:
                to_via_x(h).wait_send()
            else:
                to_via_y(lane - 2, h).wait_send()
    for rel in range(4):
        for s in range(2):
            for h in range(HALVES):
                for up in (True, False):
                    pl.when(sends(rel, s, up))(lambda up=up: y_copy(rel, s, h, up).wait_send())
                core_copy(rel, s, h).wait_send()
    for kind in range(3):
        for way in range(2):
            for h in range(HALVES):
                for j in range(CHUNKS):
                    z_copy(kind, way, h, j).wait_send()


def shards(eigvecs, slice_counts, occ_index, occ_levels):
    rows, depth = eigvecs.shape
    width = rows // CHUNKS
    dma = pltpu.SemaphoreType.DMA
    vmem = pl.BlockSpec(memory_space=pltpu.VMEM)
    return pl.pallas_call(
        kernel,
        out_shape=jax.ShapeDtypeStruct((2 * SUB, rows), F32),
        in_specs=[vmem, vmem, vmem, pl.BlockSpec(memory_space=pltpu.SMEM)],
        out_specs=vmem,
        scratch_shapes=[
            pltpu.VMEM((4, 2, 2, HALVES, HROWS, depth), F32),
            pltpu.VMEM((HALVES, HROWS, depth), F32),
            pltpu.VMEM((HALVES, HROWS, depth), F32),
            pltpu.VMEM((2, HALVES, HROWS, depth), F32),
            pltpu.VMEM((8, depth), F32),
            pltpu.VMEM((8, depth), F32),
            pltpu.VMEM((2 * CHUNKS, HROWS, depth), F32),
            pltpu.VMEM((4, 2, SUB, 2 * depth), BF16),
            pltpu.VMEM((4, 2, SUB, 2 * depth), BF16),
            pltpu.VMEM((rows, 2 * depth), BF16),
            pltpu.VMEM((rows, 2 * depth), BF16),
            pltpu.VMEM((3, 2, CHUNKS, SUB, width), F32),
            pltpu.VMEM((3, 2, CHUNKS, SUB, width), F32),
            dma((2,)),
            dma((HALVES,)),
            dma((2, HALVES)),
            dma((4, HALVES)),
            dma((2, 4, 2, HALVES)),
            dma((4, 2, HALVES)),
            dma((4, 2, 2, HALVES)),
            dma((2 * CHUNKS,)),
            dma((2 * CHUNKS,)),
            dma((3, 2, HALVES, CHUNKS)),
            dma((3, 2, HALVES, CHUNKS)),
        ],
        compiler_params=pltpu.CompilerParams(
            collective_id=0, has_side_effects=True, vmem_limit_bytes=60 * 1024 * 1024
        ),
    )(eigvecs, occ_index.reshape(1, depth), occ_levels.reshape(-1, 1), slice_counts)


def solution(mesh):
    return jax.shard_map(
        shards,
        mesh=mesh,
        in_specs=(P("row", "cuts"), P("cuts"), P("cuts"), P()),
        out_specs=P("cuts", "row"),
        check_vma=False,
    )
```

```python
import jax
import jax.numpy as jnp
from jax import lax
from jax.experimental import pallas as pl
from jax.experimental.pallas import tpu as pltpu
from jax.sharding import PartitionSpec as P

MESH = pl.DeviceIdType.MESH
SUB = 256
PIECES = 4
PROWS = SUB // PIECES
CHUNKS = 4
F32, BF16 = jnp.float32, jnp.bfloat16


def split(value):
    high = value.astype(BF16)
    return high, (value - high.astype(F32)).astype(BF16)


def kernel(
    e_any, idx_any, lev_any, cnt_any, out_ref,
    e_ref, idx_ref, lev_ref, cnt_ref, in_sem, p_buf, own_p, via_x, via_y, w_own, w_in, e_in, p_hi, p_lo, e_hi, e_lo, part, zin,
    w_sem, vx_sem, vy_sem, xs_sem, ys_sem, cs_sem, p_sem, es_sem, er_sem, zs_sem, zr_sem,
):
    rows, depth = e_ref.shape
    width = rows // CHUNKS
    c, r = lax.axis_index("cuts"), lax.axis_index("row")
    z, xl = c // 2, lax.rem(c, 2)
    q, core = r // 2, lax.rem(r, 2)
    xh, y = q // 4, lax.rem(q, 4)
    x = xh * 2 + xl

    def device(dx=0, dy=0, dz=0, dcore=0):
        nx, ny = lax.rem(x + dx + 4, 4), lax.rem(y + dy + 4, 4)
        nz, ncore = lax.rem(z + dz + 4, 4), lax.rem(core + dcore, 2)
        return (nz * 2 + lax.rem(nx, 2), ((nx // 2) * 4 + ny) * 2 + ncore)

    pair = (z * 2 + 1 - xl, r)
    other = device(dx=3 - 2 * xl)
    source = lax.rem(y, 2) == xl
    even_row = y // 2 == lax.rem(z, 2)
    bridge = jnp.logical_not(source)
    source_odd = source & jnp.logical_not(even_row)

    near_odd = jnp.where(source_odd, 1, 0)
    far_odd = 1 - near_odd

    def base(dy):
        return lax.rem(2 * xh + lax.rem(y + dy, 4) // 2 - z + 4, 4)

    own_rel = base(0)
    far_rel = lax.rem(own_rel + 2, 4)

    def row_gap(rel):
        return lax.rem(2 * lax.rem(z + rel, 2) + xl - y + 4, 4)

    barrier = pltpu.get_barrier_semaphore()
    for peer in (
        device(dx=1), device(dx=3), device(dy=1), device(dy=3),
        device(dz=1), device(dz=3), device(dcore=1),
    ):
        pl.semaphore_signal(barrier, inc=1, device_id=peer, device_id_type=MESH)

    picked, others = pl.ds(0, SUB), pl.ds(SUB, rows - SUB)
    small = [
        pltpu.make_async_copy(src, dst, in_sem.at[n])
        for n, (src, dst) in enumerate(
            ((idx_any, idx_ref), (lev_any, lev_ref), (cnt_any, cnt_ref))
        )
    ]
    load_picked = pltpu.make_async_copy(e_any.at[picked], e_ref.at[picked], in_sem.at[3])
    load_others = pltpu.make_async_copy(e_any.at[others], e_ref.at[others], in_sem.at[4])
    for load in (*small, load_picked, load_others):
        load.start()
    for load in small:
        load.wait()
    count = lev_ref.shape[1]
    diagonal = lax.broadcasted_iota(jnp.int32, (count, count), 0) == lax.broadcasted_iota(
        jnp.int32, (count, count), 1
    )
    levels = jnp.sum(jnp.where(diagonal, lev_ref[...], F32(0.0)), axis=1, keepdims=True)
    level = lax.broadcasted_iota(jnp.int32, (count, depth), 0)
    chosen = jnp.where(level == idx_ref[...], levels, F32(0.0))
    values = jnp.sum(chosen, axis=0, keepdims=True)
    live = lax.broadcasted_iota(jnp.int32, (1, depth), 1) < cnt_ref[...]
    weights = jnp.where(live, values, F32(0.0))
    w_own[...] = jnp.broadcast_to(weights, w_own.shape)
    load_picked.wait()
    for h in range(PIECES):
        own_p[h] = e_ref[h * PROWS : (h + 1) * PROWS, :] * weights

    @pl.when(source)
    def _():
        for h in range(PIECES):
            p_buf[own_rel, core, 0, h] = own_p[h]

    load_others.wait()
    pl.semaphore_wait(barrier, 7)

    def copy(src, dst, send, recv, peer):
        return pltpu.make_async_remote_copy(
            src_ref=src, dst_ref=dst, send_sem=send, recv_sem=recv,
            device_id=peer, device_id_type=MESH,
        )

    def w_copy():
        return copy(w_own, w_in, w_sem.at[0], w_sem.at[1], pair)

    def e_copy(i):
        return copy(e_ref.at[pl.ds(i * PROWS, PROWS)], e_in.at[i], es_sem, er_sem.at[i], pair)

    def slot_of(rel, s, h):
        return p_buf.at[rel, core, s, h], p_sem.at[rel, core, s, h]

    def to_via_x(h):
        return copy(own_p.at[h], via_x.at[h], xs_sem, vx_sem.at[h], other if h % 2 == 0 else pair)

    def from_via_x(h):
        slot, recv = slot_of(far_rel if h % 2 == 0 else own_rel, 0, h)
        return copy(via_x.at[h], slot, xs_sem, recv, pair if h % 2 == 0 else other)

    def to_source(h):
        slot, recv = slot_of(own_rel, 1, h)
        return copy(own_p.at[h], slot, xs_sem, recv, other)

    def to_via_y(side, h):
        return copy(
            own_p.at[h], via_y.at[side, h], xs_sem, vy_sem.at[side, h],
            device(dy=3 if side == 0 else 1),
        )

    def from_via_y(side, h):
        slot, recv = slot_of(base(1 if side == 0 else 3), 1, h)
        return copy(via_y.at[side, h], slot, xs_sem, recv, other)

    def y_copy(rel, s, h, up):
        slot, recv = slot_of(rel, s, h)
        return copy(slot, slot, ys_sem, recv, device(dy=1 if up else 3))

    def core_copy(rel, s, h):
        slot, recv = slot_of(rel, s, h)
        return copy(slot, slot, cs_sem, recv, device(dcore=1))

    def landed(ref, sem):
        pltpu.make_async_copy(ref, ref, sem).wait()

    def arrive(rel, k, s, h):
        landed(p_buf.at[rel, k, s, h], p_sem.at[rel, k, s, h])

    def spot(rel, k):
        return lax.rem(rel, 2), pl.ds(pl.multiple_of((rel // 2) * 2 * PROWS + k * PROWS, PROWS), PROWS)

    def keep(rel, k, s, h):
        high, low = split(p_buf[rel, k, s, h])
        odd, rows_of = spot(rel, k)
        p_hi[h, odd, rows_of, s * depth : (s + 1) * depth] = high
        p_lo[h, odd, rows_of, s * depth : (s + 1) * depth] = low

    def sends(rel, s, up):
        gap = row_gap(rel)
        first_hop = gap == 0
        if s == 1:
            first_hop = first_hop & (rel != far_rel)
        if up and s == 0:
            return first_hop | (gap == 3)
        if not up and s == 1:
            return first_hop | (gap == 1)
        return first_hop

    def hand_on(rel, s, h):
        for up in (True, False):
            pl.when(sends(rel, s, up))(lambda up=up: y_copy(rel, s, h, up).start())
        core_copy(rel, s, h).start()
        keep(rel, core, s, h)

    def take(rel, s, h):
        arrive(rel, core, s, h)
        hand_on(rel, s, h)

    def weigh(h):
        landed(e_in.at[h], er_sem.at[h])
        p_buf[own_rel, core, 1, h] = e_in[h] * w_in[0:1, :]
        hand_on(own_rel, 1, h)

    def need(odd, h):
        for step in range(2):
            for s in range(2):
                arrive(odd + 2 * step, 1 - core, s, h)
                keep(odd + 2 * step, 1 - core, s, h)

    def relay_x(h):
        landed(via_x.at[h], vx_sem.at[h])
        from_via_x(h).start()

    def relay_y(h):
        for side in range(2):
            landed(via_y.at[side, h], vy_sem.at[side, h])
            from_via_y(side, h).start()

    def send_rows(start, stop):
        for i in range(start, stop):
            e_copy(i).start()

    def take_far(h):
        far = base(2)
        far_next = lax.rem(far + 2, 4)
        take(far, 0, h)
        take(far, 1, h)
        take(far_next, 1, h)
        take(far_next, 0, h)

    def take_sides(h, part):
        up, down = base(1), base(3)
        up_next, down_next = lax.rem(up + 2, 4), lax.rem(down + 2, 4)
        if part == 0:
            take(up, 0, h)
            take(down, 0, h)
            take(up, 1, h)
            take(down, 1, h)
        else:
            take(up_next, 1, h)
            take(down_next, 1, h)
            take(up_next, 0, h)
            take(down_next, 0, h)

    def begin_source():
        to_via_x(0).start()
        w_copy().start()
        send_rows(0, 1)
        to_via_x(1).start()
        send_rows(1, 6)
        to_via_x(3).start()
        send_rows(6, 16)
        hand_on(own_rel, 0, 0)
        landed(w_in, w_sem.at[1])
        weigh(0)
        relay_y(0)
        to_via_x(2).start()
        take(far_rel, 1, 0)
        hand_on(own_rel, 0, 1)
        take(far_rel, 0, 0)
        weigh(1)
        relay_y(1)
        take(far_rel, 1, 1)
        take(far_rel, 0, 1)
        hand_on(own_rel, 0, 2)
        weigh(2)
        take(far_rel, 1, 2)
        relay_y(2)
        relay_y(3)
        hand_on(own_rel, 0, 3)
        weigh(3)
        take(far_rel, 1, 3)
        get_rows(0)
        near_part(0)
        near_part(1)
        take_far(0)
        need(far_odd, 0)
        half(far_odd, 0, 0)
        take(far_rel, 0, 2)
        near_part(2)
        take(far_rel, 0, 3)
        near_part(3)

    def near_part(h):
        need(near_odd, h)
        half(near_odd, h, 0)

    def begin_bridge():
        for h in range(2):
            to_source(h).start()
        for h in range(PIECES):
            for side in range(2):
                to_via_y(side, h).start()
        w_copy().start()
        send_rows(0, 1)
        relay_x(0)
        send_rows(1, 4)
        relay_x(1)
        for h in range(2, PIECES):
            to_source(h).start()
        take_sides(0, 0)
        take_sides(0, 1)
        relay_x(2)
        send_rows(4, 16)
        landed(w_in, w_sem.at[1])
        for i in range(4):
            landed(e_in.at[i], er_sem.at[i])
        get_rows(0)
        for odd in range(2):
            need(odd, 0)
            half(odd, 0, 0)
        take_sides(1, 0)
        take_sides(1, 1)
        relay_x(3)

    def split_rows(j):
        span = pl.ds(j * width, width)
        high, low = split(e_ref[span, :])
        e_hi[span, :depth] = high
        e_lo[span, :depth] = low

    def get_rows(j):
        for i in range(4 * j, 4 * j + 4):
            if j > 0:
                landed(e_in.at[i], er_sem.at[i])
            span = pl.ds(i * PROWS, PROWS)
            high, low = split(e_in[i])
            e_hi[span, depth:] = high
            e_lo[span, depth:] = low

    def dot(a, b):
        return lax.dot_general(a, b, (((1,), (1,)), ((), ())), preferred_element_type=F32)

    def z_copy(kind, way, h, j):
        rel = jnp.where(kind == 0, 2, 1 + 2 * way)
        k = jnp.where(kind == 1, 1 - way, way)
        nz = lax.rem(z + 1 + 2 * way, 4)
        odd, rows_of = spot(rel, k)
        return copy(
            part.at[h, j, odd, rows_of], zin.at[kind, way, h, j],
            zs_sem, zr_sem.at[kind, way, h, j], (nz * 2 + xl, r),
        )

    def z_landed(kind, way, h, j):
        landed(zin.at[kind, way, h, j], zr_sem.at[kind, way, h, j])

    def half(odd, h, j):
        span = pl.ds(j * width, width)
        part[h, j, odd] = dot(p_hi[h, odd], e_hi[span, :])
        part[h, j, odd] += dot(p_hi[h, odd], e_lo[span, :])
        part[h, j, odd] += dot(p_lo[h, odd], e_hi[span, :])
        for way in range(2):
            z_copy(odd, way, h, j).start()

    def both(h, j):
        half(near_odd, h, j)
        half(far_odd, h, j)

    def pass_on(h, j):
        for way in range(2):
            z_landed(0, way, h, j)
            odd, rows_of = spot(1 + 2 * way, way)
            part[h, j, odd, rows_of] += zin[0, way, h, j]
            z_copy(2, way, h, j).start()

    def finish(h, j):
        for k in range(2):
            z_landed(1, 1 - k, h, j)
            z_landed(2, k, h, j)
            odd, rows_of = spot(0, k)
            total = part[h, j, odd, rows_of] + (zin[2, k, h, j] + zin[1, 1 - k, h, j])
            out_ref[k * SUB + h * PROWS : k * SUB + (h + 1) * PROWS, j * width : (j + 1) * width] = total

    def begin():
        pl.when(source)(begin_source)
        pl.when(bridge)(begin_bridge)

    def rest(h):
        @pl.when(source)
        def _():
            take_far(h)

        @pl.when(bridge)
        def _():
            if h > 1:
                take_sides(h, 0)
                take_sides(h, 1)
            need(0, h)

        need(far_odd, h)

    def near(h, j):
        pl.when(bridge)(lambda: half(near_odd, h, j))

    def ready(h, j):
        pl.when(source)(lambda: half(near_odd, h, j))

    def far(h, j):
        half(far_odd, h, j)

    for j in range(CHUNKS):
        split_rows(j)
    begin()
    rest(1)
    near(1, 0)
    far(1, 0)
    pass_on(0, 0)
    get_rows(1)
    both(0, 1)
    pass_on(1, 0)
    both(1, 1)
    pass_on(0, 1)
    ready(2, 1)
    ready(3, 1)
    rest(2)
    near(2, 0)
    far(2, 0)
    pass_on(1, 1)
    near(2, 1)
    far(2, 1)
    pass_on(2, 0)
    get_rows(2)
    both(0, 2)
    pass_on(2, 1)
    both(1, 2)
    pass_on(0, 2)
    rest(3)
    near(3, 0)
    far(3, 0)
    pass_on(1, 2)
    near(3, 1)
    far(3, 1)
    pass_on(3, 0)
    both(2, 2)
    pass_on(3, 1)
    both(3, 2)
    pass_on(2, 2)
    get_rows(3)
    both(0, 3)
    pass_on(3, 2)
    both(1, 3)
    pass_on(0, 3)
    both(2, 3)
    pass_on(1, 3)
    both(3, 3)
    pass_on(2, 3)
    for j in range(CHUNKS - 1):
        for h in range(PIECES):
            finish(h, j)
    pass_on(3, 3)
    for h in range(PIECES):
        finish(h, CHUNKS - 1)

    w_copy().wait_send()
    landed(e_ref, es_sem)
    landed(p_buf.at[pl.ds(0, 2)], cs_sem)
    landed(zin, zs_sem)

    @pl.when(source)
    def _():
        landed(p_buf.at[pl.ds(0, 3), 0, 0], xs_sem)
        landed(p_buf.at[pl.ds(0, 3), 0], ys_sem)

    @pl.when(bridge)
    def _():
        landed(p_buf.at[0], xs_sem)
        landed(p_buf.at[0], ys_sem)


def shards(eigvecs, slice_counts, occ_index, occ_levels):
    rows, depth = eigvecs.shape
    width = rows // CHUNKS
    dma = pltpu.SemaphoreType.DMA
    levels = occ_levels.shape[0]
    return pl.pallas_call(
        kernel,
        out_shape=pltpu.VMEM((2 * SUB, rows), F32),
        in_specs=[pl.BlockSpec(memory_space=pl.ANY)] * 4,
        out_specs=pl.BlockSpec(memory_space=pltpu.VMEM),
        scratch_shapes=[
            pltpu.VMEM((rows, depth), F32),
            pltpu.VMEM((1, depth), jnp.int32),
            pltpu.VMEM((1, levels), F32),
            pltpu.VMEM((1, 1), jnp.int32),
            dma((5,)),
            pltpu.VMEM((4, 2, 2, PIECES, PROWS, depth), F32),
            pltpu.VMEM((PIECES, PROWS, depth), F32),
            pltpu.VMEM((PIECES, PROWS, depth), F32),
            pltpu.VMEM((2, PIECES, PROWS, depth), F32),
            pltpu.VMEM((8, depth), F32),
            pltpu.VMEM((8, depth), F32),
            pltpu.VMEM((rows // PROWS, PROWS, depth), F32),
            pltpu.VMEM((PIECES, 2, 4 * PROWS, 2 * depth), BF16),
            pltpu.VMEM((PIECES, 2, 4 * PROWS, 2 * depth), BF16),
            pltpu.VMEM((rows, 2 * depth), BF16),
            pltpu.VMEM((rows, 2 * depth), BF16),
            pltpu.VMEM((PIECES, CHUNKS, 2, 4 * PROWS, width), F32),
            pltpu.VMEM((3, 2, PIECES, CHUNKS, PROWS, width), F32),
            dma((2,)),
            dma((PIECES,)),
            dma((2, PIECES)),
            dma,
            dma,
            dma,
            dma((4, 2, 2, PIECES)),
            dma,
            dma((rows // PROWS,)),
            dma,
            dma((3, 2, PIECES, CHUNKS)),
        ],
        compiler_params=pltpu.CompilerParams(
            collective_id=0, has_side_effects=True, vmem_limit_bytes=60 * 1024 * 1024
        ),
    )(
        eigvecs,
        occ_index.reshape(1, depth),
        occ_levels.reshape(1, levels),
        slice_counts.reshape(1, 1),
    )


def solution(mesh):
    return jax.shard_map(
        shards,
        mesh=mesh,
        in_specs=(P("row", "cuts"), P("cuts"), P("cuts"), P()),
        out_specs=P("cuts", "row"),
        check_vma=False,
    )
```

```python
import jax
import jax.numpy as jnp
from jax import lax
from jax.experimental import pallas as pl
from jax.experimental.pallas import tpu as pltpu
from jax.sharding import PartitionSpec as P

MESH = pl.DeviceIdType.MESH
SUB = 256
PIECES = 4
PROWS = SUB // PIECES
WIDE = 128
FIRST, SECOND, THIRD, FOURTH = (0, 2), (2, 2), (4, 2), (6, 2)
SECOND_A, SECOND_B = (2, 1), (3, 1)
F32, BF16 = jnp.float32, jnp.bfloat16


def split(value):
    high = value.astype(BF16)
    return high, (value - high.astype(F32)).astype(BF16)


def kernel(
    e_any, idx_any, lev_any, cnt_any, out_ref,
    e_ref, idx_ref, lev_ref, cnt_ref, in_sem, p_buf, own_p, via_x, via_y, w_own, w_in, e_in, p_hi, p_lo, e_hi, e_lo, part, first_in, second_in, third_in,
    w_sem, vx_sem, vy_sem, xs_sem, ys_sem, cs_sem, p_sem, es_sem, er_sem, zs_sem, first_sem, later_sem,
):
    rows, depth = e_ref.shape
    c, r = lax.axis_index("cuts"), lax.axis_index("row")
    z, xl = c // 2, lax.rem(c, 2)
    q, core = r // 2, lax.rem(r, 2)
    xh, y = q // 4, lax.rem(q, 4)
    x = xh * 2 + xl

    def device(dx=0, dy=0, dz=0, dcore=0):
        nx, ny = lax.rem(x + dx + 4, 4), lax.rem(y + dy + 4, 4)
        nz, ncore = lax.rem(z + dz + 4, 4), lax.rem(core + dcore, 2)
        return (nz * 2 + lax.rem(nx, 2), ((nx // 2) * 4 + ny) * 2 + ncore)

    pair = (z * 2 + 1 - xl, r)
    other = device(dx=3 - 2 * xl)
    source = lax.rem(y, 2) == xl
    even_row = y // 2 == lax.rem(z, 2)
    bridge = jnp.logical_not(source)
    source_odd = source & jnp.logical_not(even_row)

    source_even = source & even_row
    not_odd = jnp.logical_not(source_odd)

    def base(dy):
        return lax.rem(2 * xh + lax.rem(y + dy, 4) // 2 - z + 4, 4)

    own_rel = base(0)
    far_rel = lax.rem(own_rel + 2, 4)

    def row_gap(rel):
        return lax.rem(2 * lax.rem(z + rel, 2) + xl - y + 4, 4)

    barrier = pltpu.get_barrier_semaphore()
    for peer in (
        device(dx=1), device(dx=2), device(dx=3), device(dy=1), device(dy=3),
        device(dz=1), device(dz=3), device(dcore=1),
    ):
        pl.semaphore_signal(barrier, inc=1, device_id=peer, device_id_type=MESH)

    picked, others = pl.ds(0, SUB), pl.ds(SUB, rows - SUB)
    small = [
        pltpu.make_async_copy(src, dst, in_sem.at[n])
        for n, (src, dst) in enumerate(
            ((idx_any, idx_ref), (lev_any, lev_ref), (cnt_any, cnt_ref))
        )
    ]
    load_picked = pltpu.make_async_copy(e_any.at[picked], e_ref.at[picked], in_sem.at[3])
    load_others = pltpu.make_async_copy(e_any.at[others], e_ref.at[others], in_sem.at[4])
    for load in (*small, load_picked, load_others):
        load.start()
    for load in small:
        load.wait()
    count = lev_ref.shape[1]
    diagonal = lax.broadcasted_iota(jnp.int32, (count, count), 0) == lax.broadcasted_iota(
        jnp.int32, (count, count), 1
    )
    levels = jnp.sum(jnp.where(diagonal, lev_ref[...], F32(0.0)), axis=1, keepdims=True)
    level = lax.broadcasted_iota(jnp.int32, (count, depth), 0)
    chosen = jnp.where(level == idx_ref[...], levels, F32(0.0))
    values = jnp.sum(chosen, axis=0, keepdims=True)
    live = lax.broadcasted_iota(jnp.int32, (1, depth), 1) < cnt_ref[...]
    weights = jnp.where(live, values, F32(0.0))
    w_own[...] = jnp.broadcast_to(weights, w_own.shape)
    load_picked.wait()
    for h in range(PIECES):
        own_p[h] = e_ref[h * PROWS : (h + 1) * PROWS, :] * weights

    @pl.when(source)
    def _():
        for h in range(PIECES):
            p_buf[own_rel, core, 0, h] = own_p[h]

    load_others.wait()
    for i in range(4):
        span = pl.ds(i * SUB, SUB)
        high, low = split(e_ref[span, :])
        e_hi[span, :depth] = high
        e_lo[span, :depth] = low
    pl.semaphore_wait(barrier, 8)

    def copy(src, dst, send, recv, peer):
        return pltpu.make_async_remote_copy(
            src_ref=src, dst_ref=dst, send_sem=send, recv_sem=recv,
            device_id=peer, device_id_type=MESH,
        )

    def w_copy():
        return copy(w_own, w_in, w_sem.at[0], w_sem.at[1], pair)

    def e_copy(i):
        return copy(e_ref.at[pl.ds(i * PROWS, PROWS)], e_in.at[i], es_sem, er_sem.at[i], pair)

    def slot_of(rel, s, h):
        return p_buf.at[rel, core, s, h], p_sem.at[rel, core, s, h]

    def to_twin(h):
        slot, recv = slot_of(own_rel, 0, h)
        return copy(own_p.at[h], slot, xs_sem, recv, device(dx=2))

    def to_via_x(h):
        peer = pair if h == 2 else other
        return copy(own_p.at[h], via_x.at[h - 1], xs_sem, vx_sem.at[h - 1], peer)

    def from_via_x(h):
        slot, recv = slot_of(own_rel if h == 2 else far_rel, 0, h)
        return copy(via_x.at[h - 1], slot, xs_sem, recv, other if h == 2 else pair)

    def to_source(h):
        slot, recv = slot_of(own_rel, 1, h)
        return copy(own_p.at[h], slot, xs_sem, recv, other)

    def to_via_y(side, h):
        return copy(
            own_p.at[h], via_y.at[side, h], xs_sem, vy_sem.at[side, h],
            device(dy=3 if side == 0 else 1),
        )

    def from_via_y(side, h):
        slot, recv = slot_of(base(1 if side == 0 else 3), 1, h)
        return copy(via_y.at[side, h], slot, xs_sem, recv, other)

    def y_copy(rel, s, h, up):
        slot, recv = slot_of(rel, s, h)
        return copy(slot, slot, ys_sem, recv, device(dy=1 if up else 3))

    def core_copy(rel, s, h):
        slot, recv = slot_of(rel, s, h)
        return copy(slot, slot, cs_sem, recv, device(dcore=1))

    def landed(ref, sem):
        pltpu.make_async_copy(ref, ref, sem).wait()

    def arrive(rel, k, s, h):
        landed(p_buf.at[rel, k, s, h], p_sem.at[rel, k, s, h])

    def spot(rel, k, h):
        odd = lax.rem(rel, 2)
        block = jnp.where(odd == 1, 2 + h, jnp.where(rel == 2, h // 2, 6 + k))
        row = jnp.where(
            odd == 1,
            (rel // 2) * 2 * PROWS + k * PROWS,
            jnp.where(rel == 2, k * 2 * PROWS + lax.rem(h, 2) * PROWS, h * PROWS),
        )
        return block, pl.ds(pl.multiple_of(row, PROWS), PROWS)

    def keep(rel, k, s, h):
        high, low = split(p_buf[rel, k, s, h])
        block, rows_of = spot(rel, k, h)
        p_hi[block, rows_of, s * depth : (s + 1) * depth] = high
        p_lo[block, rows_of, s * depth : (s + 1) * depth] = low

    def sends(rel, s, up):
        gap = row_gap(rel)
        first_hop = gap == 0
        if s == 1:
            first_hop = first_hop & (rel != far_rel)
        if up and s == 0:
            return first_hop | (gap == 3)
        if not up and s == 1:
            return first_hop | (gap == 1)
        return first_hop

    def hand_on(rel, s, h):
        for up in (True, False):
            pl.when(sends(rel, s, up))(lambda up=up: y_copy(rel, s, h, up).start())
        core_copy(rel, s, h).start()
        keep(rel, core, s, h)

    def take(rel, s, h):
        arrive(rel, core, s, h)
        hand_on(rel, s, h)

    def weigh(h, wait=True):
        if wait:
            landed(e_in.at[h], er_sem.at[h])
        p_buf[own_rel, core, 1, h] = e_in[h] * w_in[0:1, :]
        hand_on(own_rel, 1, h)

    def need(rel, h):
        for s in range(2):
            arrive(rel, 1 - core, s, h)
            keep(rel, 1 - core, s, h)

    def need_odd(h):
        need(1, h)
        need(3, h)

    def relay_x(h):
        landed(via_x.at[h - 1], vx_sem.at[h - 1])
        from_via_x(h).start()

    def relay_y(h):
        for side in range(2):
            landed(via_y.at[side, h], vy_sem.at[side, h])
            from_via_y(side, h).start()

    def send_rows(start, stop):
        for i in range(start, stop):
            e_copy(i).start()

    def take_pair(rel, h):
        take(rel, 0, h)
        take(rel, 1, h)

    odd_rel = jnp.where(lax.rem(base(1), 2) == 1, base(1), base(3))
    odd_rel = jnp.where(source, base(2), odd_rel)

    def take_odd(h):
        take_pair(odd_rel, h)
        take_pair(lax.rem(odd_rel + 2, 4), h)

    def begin_source():
        to_twin(0).start()
        to_via_x(1).start()
        to_via_x(3).start()
        w_copy().start()
        send_rows(0, 2)
        to_via_x(2).start()
        send_rows(2, 16)
        hand_on(own_rel, 0, 0)

        @pl.when(source_odd)
        def _():
            hand_on(own_rel, 0, 1)
            landed(w_in, w_sem.at[1])
            weigh(0)
            relay_y(0)
            take(far_rel, 1, 0)
            take(far_rel, 0, 0)
            weigh(1)
            relay_y(1)
            take(far_rel, 1, 1)
            take(far_rel, 0, 1)
            relay_y(2)
            hand_on(own_rel, 0, 2)
            weigh(2)
            relay_y(3)
            landed(e_in.at[3], er_sem.at[3])
            get_rows(0, 4)
            need_odd(0)
            second(0, FIRST)
            need_odd(1)
            second(1, FIRST)
            take(far_rel, 1, 2)
            take(far_rel, 0, 2)
            hand_on(own_rel, 0, 3)
            weigh(3, False)
            need_odd(2)
            second(2, FIRST)
            take(far_rel, 1, 3)
            take(far_rel, 0, 3)
            need_odd(3)
            second(3, FIRST)
            third(0, FIRST)
            third(1, FIRST)
            take_pair(2, 0)
            take_pair(2, 1)
            need(2, 0)
            need(2, 1)
            first(0, FIRST)
            third(2, FIRST)
            third(3, FIRST)
            get_rows(4, 6)
            first(0, SECOND_A)
            second(0, SECOND_A)
            second(1, SECOND_A)
            get_rows(6, 8)
            first(0, SECOND_B)
            second(0, SECOND_B)
            second(1, SECOND_B)
            second(2, SECOND)
            second(3, SECOND)
            for h in (2, 3):
                take_pair(2, h)
                need(2, h)
            first(1, FIRST)
            first(1, SECOND)

        @pl.when(source_even & (own_rel == 2))
        def _():
            hand_on(own_rel, 0, 1)
            landed(w_in, w_sem.at[1])
            weigh(0)
            relay_y(0)
            weigh(1)
            relay_y(1)
            hand_on(own_rel, 0, 2)
            relay_y(2)
            weigh(2)
            relay_y(3)
            hand_on(own_rel, 0, 3)
            weigh(3)
            get_rows(0, 4)
            for two in range(2):
                need(2, 2 * two)
                need(2, 2 * two + 1)
                first(two, FIRST)
            for h in range(PIECES):
                take(far_rel, 1, h)
                take(far_rel, 0, h)

        @pl.when(source_even & (own_rel == 0))
        def _():
            hand_on(own_rel, 0, 1)
            hand_on(own_rel, 0, 2)
            landed(w_in, w_sem.at[1])
            relay_y(0)
            take_pair(far_rel, 0)
            relay_y(1)
            weigh(0)
            take_pair(far_rel, 1)
            relay_y(2)
            relay_y(3)
            for h in range(1, PIECES):
                landed(e_in.at[h], er_sem.at[h])
            get_rows(0, 4)
            need(2, 0)
            need(2, 1)
            first(0, FIRST)
            take_pair(far_rel, 2)
            take_pair(far_rel, 3)
            need(2, 2)
            need(2, 3)
            first(1, FIRST)
            hand_on(own_rel, 0, 3)
            for h in range(1, PIECES):
                weigh(h, False)

        @pl.when(source_even)
        def _():
            get_rows(4, 6)
            first(0, SECOND_A)
            take_odd(0)
            need_odd(0)
            second(0, FIRST)
            second(0, SECOND_A)
            get_rows(6, 8)
            first(0, SECOND_B)
            second(0, SECOND_B)
            first(1, SECOND)
            take_odd(1)
            need_odd(1)
            second(1, FIRST)
            second(1, SECOND_A)
            second(1, SECOND_B)
            third(0, FIRST)
            third(1, FIRST)
            third(0, SECOND_A)
            third(1, SECOND_A)
            get_rows(8, 12)
            first(0, THIRD)
            first(1, THIRD)
            take_odd(2)
            need_odd(2)
            second(2, FIRST)
            second(2, SECOND)

    def begin_bridge():
        for h in range(2):
            to_source(h).start()
        for h in range(PIECES):
            for side in range(2):
                to_via_y(side, h).start()
        w_copy().start()
        send_rows(0, 2)
        relay_x(1)
        send_rows(2, 4)
        relay_x(3)
        send_rows(4, 16)
        for h in range(2, PIECES):
            to_source(h).start()
        odd_next = lax.rem(odd_rel + 2, 4)
        take_pair(odd_rel, 0)
        relay_x(2)
        take_pair(2, 0)
        take_pair(odd_next, 0)
        landed(w_in, w_sem.at[1])
        for i in range(4):
            landed(e_in.at[i], er_sem.at[i])
        get_rows(0, 4)
        need_odd(0)
        second(0, FIRST)
        take_pair(2, 1)
        need(2, 0)
        need(2, 1)
        first(0, FIRST)
        take_pair(odd_rel, 1)
        get_rows(4, 6)
        first(0, SECOND_A)
        second(0, SECOND_A)
        take_pair(odd_next, 1)
        need_odd(1)
        second(1, FIRST)
        second(1, SECOND_A)
        take_pair(2, 2)
        third(0, FIRST)
        third(1, FIRST)
        take_pair(2, 3)
        need(2, 2)
        need(2, 3)
        first(1, FIRST)
    def get_rows(start, stop):
        for i in range(start, stop):
            if start > 0:
                landed(e_in.at[i], er_sem.at[i])
            span = pl.ds(i * PROWS, PROWS)
            high, low = split(e_in[i])
            e_hi[span, depth:] = high
            e_lo[span, depth:] = low

    def dot(a, b):
        return lax.dot_general(a, b, (((1,), (1,)), ((), ())), preferred_element_type=F32)

    def ring(way):
        return (lax.rem(z + 1 + 2 * way, 4) * 2 + xl, r)

    def first_copy(way, two, chunk):
        slots = pl.ds(*chunk)
        return copy(
            part.at[two, slots, pl.ds(2 * way * PROWS, 2 * PROWS)], first_in.at[way, two, slots],
            zs_sem, first_sem.at[way, two, chunk[0]], ring(way),
        )

    def second_copy(way, h, chunk):
        slots = pl.ds(*chunk)
        return copy(
            part.at[2 + h, slots, pl.ds((1 + way) * PROWS, PROWS)], second_in.at[way, h, slots],
            zs_sem, later_sem.at[0, way, h, chunk[0]], ring(way),
        )

    def third_copy(way, h, chunk):
        slots = pl.ds(*chunk)
        return copy(
            part.at[2 + h, slots, pl.ds(3 * way * PROWS, PROWS)], third_in.at[way, h, slots],
            zs_sem, later_sem.at[1, way, h, chunk[0]], ring(way),
        )

    here = z >= 0

    def product(block, chunk):
        span = pl.ds(chunk[0] * WIDE, chunk[1] * WIDE)
        total = dot(p_hi[block], e_hi[span, :])
        total += dot(p_hi[block], e_lo[span, :])
        total += dot(p_lo[block], e_hi[span, :])
        for i in range(chunk[1]):
            part[block, chunk[0] + i] = total[:, i * WIDE : (i + 1) * WIDE]

    def first(two, chunk):
        pl.when(here)(lambda: product(two, chunk))
        for way in range(2):
            first_copy(way, two, chunk).start()

    def second(h, chunk):
        pl.when(here)(lambda: product(2 + h, chunk))
        for way in range(2):
            second_copy(way, h, chunk).start()

    def third(h, chunk):
        slots = pl.ds(*chunk)
        for way in range(2):
            if h % 2 == 0:
                landed(first_in.at[way, h // 2, slots], first_sem.at[way, h // 2, chunk[0]])
            low = (h % 2) * PROWS
            for i in range(chunk[0], chunk[0] + chunk[1]):
                part[2 + h, i, 3 * way * PROWS : (3 * way + 1) * PROWS] += first_in[
                    way, h // 2, i, low : low + PROWS
                ]
            third_copy(way, h, chunk).start()

    def last(chunk):
        pl.when(here)(lambda: product(6, chunk))
        pl.when(here)(lambda: product(7, chunk))

    def finish(h, chunk):
        slots = pl.ds(*chunk)
        for k in range(2):
            landed(second_in.at[1 - k, h, slots], later_sem.at[0, 1 - k, h, chunk[0]])
            landed(third_in.at[k, h, slots], later_sem.at[1, k, h, chunk[0]])
            top = k * SUB + h * PROWS
            for i in range(chunk[0], chunk[0] + chunk[1]):
                total = part[6 + k, i, h * PROWS : (h + 1) * PROWS]
                total += third_in[k, h, i] + second_in[1 - k, h, i]
                out_ref[top : top + PROWS, i * WIDE : (i + 1) * WIDE] = total

    def begin():
        pl.when(source)(begin_source)
        pl.when(bridge)(begin_bridge)

    def more(h):
        @pl.when(bridge if h == 2 else not_odd)
        def _():
            take_odd(h)
            need_odd(h)
            second(h, FIRST)
            second(h, SECOND)

    def pass_own():
        @pl.when(bridge)
        def _():
            for h in range(PIECES):
                take_pair(0, h)

    def own_parts():
        @pl.when(source_odd)
        def _():
            for h in range(PIECES):
                take_pair(0, h)

        for h in range(PIECES):
            need(0, h)

    def middle():
        @pl.when(bridge)
        def _():
            get_rows(6, 8)
            first(0, SECOND_B)
            second(0, SECOND_B)
            first(1, SECOND)
            second(1, SECOND_B)

    def now_third():
        @pl.when(jnp.logical_not(source_even))
        def _():
            third(0, SECOND_A)
            third(1, SECOND_A)

    def now_first():
        @pl.when(jnp.logical_not(source_even))
        def _():
            get_rows(8, 12)
            first(0, THIRD)
            first(1, THIRD)

    def middle_third():
        @pl.when(not_odd)
        def _():
            third(2, FIRST)
            third(3, FIRST)

    begin()
    middle()
    more(2)
    now_third()
    third(0, SECOND_B)
    third(1, SECOND_B)
    now_first()
    more(3)
    pass_own()
    middle_third()
    third(2, SECOND)
    third(3, SECOND)
    for h in range(PIECES):
        second(h, THIRD)
    get_rows(12, 16)
    first(0, FOURTH)
    first(1, FOURTH)
    third(0, THIRD)
    third(1, THIRD)
    second(0, FOURTH)
    third(2, THIRD)
    second(1, FOURTH)
    third(3, THIRD)
    second(2, FOURTH)
    second(3, FOURTH)
    own_parts()
    for chunk in (FIRST, SECOND, THIRD, FOURTH):
        last(chunk)
    for h in range(PIECES):
        third(h, FOURTH)
    for h in range(PIECES):
        for chunk in (FIRST, *((SECOND_A, SECOND_B) if h < 2 else (SECOND,)), THIRD):
            finish(h, chunk)
    for h in range(PIECES):
        finish(h, FOURTH)

    w_copy().wait_send()
    landed(e_ref, es_sem)
    landed(p_buf.at[pl.ds(0, 2)], cs_sem)
    landed(p_buf.at[pl.ds(0, 3)], zs_sem)

    @pl.when(source)
    def _():
        landed(p_buf.at[pl.ds(0, 3), 0, 0], xs_sem)
        landed(p_buf.at[pl.ds(0, 3), 0], ys_sem)

    @pl.when(bridge)
    def _():
        landed(p_buf.at[pl.ds(0, 3), 0, 0], xs_sem)
        landed(via_x, xs_sem)
        landed(p_buf.at[0], ys_sem)


def shards(eigvecs, slice_counts, occ_index, occ_levels):
    rows, depth = eigvecs.shape
    dma = pltpu.SemaphoreType.DMA
    levels = occ_levels.shape[0]
    slots = rows // WIDE
    return pl.pallas_call(
        kernel,
        out_shape=pltpu.VMEM((2 * SUB, rows), F32),
        in_specs=[pl.BlockSpec(memory_space=pl.ANY)] * 4,
        out_specs=pl.BlockSpec(memory_space=pltpu.VMEM),
        scratch_shapes=[
            pltpu.VMEM((rows, depth), F32),
            pltpu.VMEM((1, depth), jnp.int32),
            pltpu.VMEM((1, levels), F32),
            pltpu.VMEM((1, 1), jnp.int32),
            dma((5,)),
            pltpu.VMEM((4, 2, 2, PIECES, PROWS, depth), F32),
            pltpu.VMEM((PIECES, PROWS, depth), F32),
            pltpu.VMEM((PIECES - 1, PROWS, depth), F32),
            pltpu.VMEM((2, PIECES, PROWS, depth), F32),
            pltpu.VMEM((8, depth), F32),
            pltpu.VMEM((8, depth), F32),
            pltpu.VMEM((rows // PROWS, PROWS, depth), F32),
            pltpu.VMEM((8, SUB, 2 * depth), BF16),
            pltpu.VMEM((8, SUB, 2 * depth), BF16),
            pltpu.VMEM((rows, 2 * depth), BF16),
            pltpu.VMEM((rows, 2 * depth), BF16),
            pltpu.VMEM((8, slots, SUB, WIDE), F32),
            pltpu.VMEM((2, 2, slots, 2 * PROWS, WIDE), F32),
            pltpu.VMEM((2, PIECES, slots, PROWS, WIDE), F32),
            pltpu.VMEM((2, PIECES, slots, PROWS, WIDE), F32),
            dma((2,)),
            dma((PIECES - 1,)),
            dma((2, PIECES)),
            dma,
            dma,
            dma,
            dma((4, 2, 2, PIECES)),
            dma,
            dma((rows // PROWS,)),
            dma,
            dma((2, 2, slots)),
            dma((2, 2, PIECES, slots)),
        ],
        compiler_params=pltpu.CompilerParams(
            collective_id=0, has_side_effects=True, vmem_limit_bytes=60 * 1024 * 1024
        ),
    )(
        eigvecs,
        occ_index.reshape(1, depth),
        occ_levels.reshape(1, levels),
        slice_counts.reshape(1, 1),
    )


def solution(mesh):
    return jax.shard_map(
        shards,
        mesh=mesh,
        in_specs=(P("row", "cuts"), P("cuts"), P("cuts"), P()),
        out_specs=P("cuts", "row"),
        check_vma=False,
    )
```

```python
import jax
import jax.numpy as jnp
from jax import lax
from jax.experimental import pallas as pl
from jax.experimental.pallas import tpu as pltpu
from jax.sharding import PartitionSpec as P

MESH = pl.DeviceIdType.MESH
SUB = 256
PIECES = 4
PROWS = SUB // PIECES
WIDE = 128
FIRST, SECOND, THIRD, FOURTH = (0, 2), (2, 2), (4, 2), (6, 2)
SECOND_A, SECOND_B = (2, 1), (3, 1)
SLOTS = (0, 2, 3, 4, 6)
F32, BF16 = jnp.float32, jnp.bfloat16


def split(value):
    high = value.astype(BF16)
    return high, (value - high.astype(F32)).astype(BF16)


def kernel(
    e_any, idx_any, lev_any, cnt_any, out_ref,
    e_ref, idx_ref, lev_ref, cnt_ref, in_sem, p_buf, own_p, via_x, via_y, w_own, w_in, e_in, p_hi, p_lo, e_hi, e_lo, part, first_in, second_in, third_in,
    w_sem, vx_sem, vy_sem, xs_sem, ys_sem, cs_sem, p_sem, es_sem, er_sem, zs_sem, first_sem, later_sem,
):
    rows, depth = e_ref.shape
    c, r = lax.axis_index("cuts"), lax.axis_index("row")
    z, xl = c // 2, lax.rem(c, 2)
    q, core = r // 2, lax.rem(r, 2)
    xh, y = q // 4, lax.rem(q, 4)
    x = xh * 2 + xl

    def device(dx=0, dy=0, dz=0, dcore=0):
        nx, ny = lax.rem(x + dx + 4, 4), lax.rem(y + dy + 4, 4)
        nz, ncore = lax.rem(z + dz + 4, 4), lax.rem(core + dcore, 2)
        return (nz * 2 + lax.rem(nx, 2), ((nx // 2) * 4 + ny) * 2 + ncore)

    pair = (z * 2 + 1 - xl, r)
    other = device(dx=3 - 2 * xl)
    source = lax.rem(y, 2) == xl
    even_row = y // 2 == lax.rem(z, 2)
    bridge = jnp.logical_not(source)
    source_odd = source & jnp.logical_not(even_row)

    source_even = source & even_row
    not_odd = jnp.logical_not(source_odd)

    def base(dy):
        return lax.rem(2 * xh + lax.rem(y + dy, 4) // 2 - z + 4, 4)

    own_rel = base(0)
    far_rel = lax.rem(own_rel + 2, 4)

    def row_gap(rel):
        return lax.rem(2 * lax.rem(z + rel, 2) + xl - y + 4, 4)

    barrier = pltpu.get_barrier_semaphore()
    for peer in (
        device(dx=1), device(dx=2), device(dx=3), device(dy=1), device(dy=3),
        device(dz=1), device(dz=3), device(dcore=1),
    ):
        pl.semaphore_signal(barrier, inc=1, device_id=peer, device_id_type=MESH)

    picked, others = pl.ds(0, SUB), pl.ds(SUB, rows - SUB)
    small = [
        pltpu.make_async_copy(src, dst, in_sem.at[n])
        for n, (src, dst) in enumerate(
            ((idx_any, idx_ref), (lev_any, lev_ref), (cnt_any, cnt_ref))
        )
    ]
    load_picked = pltpu.make_async_copy(e_any.at[picked], e_ref.at[picked], in_sem.at[3])
    load_others = pltpu.make_async_copy(e_any.at[others], e_ref.at[others], in_sem.at[4])
    for load in (*small, load_picked, load_others):
        load.start()
    for load in small:
        load.wait()
    count = lev_ref.shape[1]
    diagonal = lax.broadcasted_iota(jnp.int32, (count, count), 0) == lax.broadcasted_iota(
        jnp.int32, (count, count), 1
    )
    levels = jnp.sum(jnp.where(diagonal, lev_ref[...], F32(0.0)), axis=1, keepdims=True)
    level = lax.broadcasted_iota(jnp.int32, (count, depth), 0)
    chosen = jnp.where(level == idx_ref[...], levels, F32(0.0))
    values = jnp.sum(chosen, axis=0, keepdims=True)
    live = lax.broadcasted_iota(jnp.int32, (1, depth), 1) < cnt_ref[...]
    weights = jnp.where(live, values, F32(0.0))
    w_own[...] = jnp.broadcast_to(weights, w_own.shape)
    load_picked.wait()
    for h in range(PIECES):
        own_p[h] = e_ref[h * PROWS : (h + 1) * PROWS, :] * weights

    @pl.when(source)
    def _():
        for h in range(PIECES):
            p_buf[own_rel, core, 0, h] = own_p[h]

    pl.semaphore_wait(barrier, 8)

    def copy(src, dst, send, recv, peer):
        return pltpu.make_async_remote_copy(
            src_ref=src, dst_ref=dst, send_sem=send, recv_sem=recv,
            device_id=peer, device_id_type=MESH,
        )

    def w_copy():
        return copy(w_own, w_in, w_sem.at[0], w_sem.at[1], pair)

    def e_copy(i):
        return copy(e_ref.at[pl.ds(i * PROWS, PROWS)], e_in.at[i], es_sem, er_sem.at[i], pair)

    def slot_of(rel, s, h):
        return p_buf.at[rel, core, s, h], p_sem.at[rel, core, s, h]

    def to_twin(h):
        slot, recv = slot_of(own_rel, 0, h)
        return copy(own_p.at[h], slot, xs_sem, recv, device(dx=2))

    def to_via_x(h):
        return copy(own_p.at[h], via_x.at[h // 2], xs_sem, vx_sem.at[h // 2], other)

    def from_via_x(h):
        slot, recv = slot_of(far_rel, 0, h)
        return copy(via_x.at[h // 2], slot, xs_sem, recv, pair)

    def to_source(h):
        slot, recv = slot_of(own_rel, 1, h)
        return copy(own_p.at[h], slot, xs_sem, recv, other)

    def to_via_y(side, h):
        return copy(
            own_p.at[h], via_y.at[side, h], xs_sem, vy_sem.at[side, h],
            device(dy=3 if side == 0 else 1),
        )

    def from_via_y(side, h):
        slot, recv = slot_of(base(1 if side == 0 else 3), 1, h)
        return copy(via_y.at[side, h], slot, xs_sem, recv, other)

    def y_copy(rel, s, h, up):
        slot, recv = slot_of(rel, s, h)
        return copy(slot, slot, ys_sem, recv, device(dy=1 if up else 3))

    def core_copy(rel, s, h):
        slot, recv = slot_of(rel, s, h)
        return copy(slot, slot, cs_sem, recv, device(dcore=1))

    def landed(ref, sem):
        pltpu.make_async_copy(ref, ref, sem).wait()

    def arrive(rel, k, s, h):
        landed(p_buf.at[rel, k, s, h], p_sem.at[rel, k, s, h])

    def spot(rel, k, h):
        odd = lax.rem(rel, 2)
        block = jnp.where(odd == 1, 2 + h, jnp.where(rel == 2, h // 2, 6 + k))
        row = jnp.where(
            odd == 1,
            (rel // 2) * 2 * PROWS + k * PROWS,
            jnp.where(rel == 2, lax.rem(h, 2) * 2 * PROWS + k * PROWS, h * PROWS),
        )
        return block, pl.ds(pl.multiple_of(row, PROWS), PROWS)

    def keep(rel, k, s, h):
        high, low = split(p_buf[rel, k, s, h])
        block, rows_of = spot(rel, k, h)
        p_hi[block, rows_of, s * depth : (s + 1) * depth] = high
        p_lo[block, rows_of, s * depth : (s + 1) * depth] = low

    def sends(rel, s, up):
        gap = row_gap(rel)
        first_hop = gap == 0
        if s == 1:
            first_hop = first_hop & (rel != far_rel)
        if up and s == 0:
            return first_hop | (gap == 3)
        if not up and s == 1:
            return first_hop | (gap == 1)
        return first_hop

    def hand_on(rel, s, h):
        for up in (True, False):
            pl.when(sends(rel, s, up))(lambda up=up: y_copy(rel, s, h, up).start())
        core_copy(rel, s, h).start()
        keep(rel, core, s, h)

    def take(rel, s, h):
        arrive(rel, core, s, h)
        hand_on(rel, s, h)

    def weigh(h, wait=True):
        if wait:
            landed(e_in.at[h], er_sem.at[h])
        p_buf[own_rel, core, 1, h] = e_in[h] * w_in[0:1, :]
        hand_on(own_rel, 1, h)

    def need(rel, h):
        for s in range(2):
            arrive(rel, 1 - core, s, h)
            keep(rel, 1 - core, s, h)

    def need_odd(h):
        need(1, h)
        need(3, h)

    def relay_x(h):
        landed(via_x.at[h // 2], vx_sem.at[h // 2])
        from_via_x(h).start()

    def relay_y(h):
        for side in range(2):
            landed(via_y.at[side, h], vy_sem.at[side, h])
            from_via_y(side, h).start()

    def send_rows(start, stop):
        for i in range(start, stop):
            e_copy(i).start()

    def take_pair(rel, h):
        take(rel, 0, h)
        take(rel, 1, h)

    odd_rel = jnp.where(lax.rem(base(1), 2) == 1, base(1), base(3))
    odd_rel = jnp.where(source, base(2), odd_rel)

    def take_odd(h):
        take_pair(odd_rel, h)
        take_pair(lax.rem(odd_rel + 2, 4), h)

    def send_others():
        load_others.wait()
        send_rows(4, 16)
        for i in range(4):
            span = pl.ds(i * SUB, SUB)
            high, low = split(e_ref[span, :])
            e_hi[span, :depth] = high
            e_lo[span, :depth] = low

    def begin_source():
        to_twin(0).start()
        to_via_x(1).start()
        to_via_x(3).start()
        w_copy().start()
        send_rows(0, 4)
        to_twin(2).start()
        hand_on(own_rel, 0, 0)
        send_others()

        @pl.when(source_odd)
        def _():
            hand_on(own_rel, 0, 1)
            landed(w_in, w_sem.at[1])
            weigh(0)
            relay_y(0)
            take(far_rel, 1, 0)
            take(far_rel, 0, 0)
            weigh(1)
            relay_y(1)
            take(far_rel, 1, 1)
            take(far_rel, 0, 1)
            relay_y(2)
            hand_on(own_rel, 0, 2)
            weigh(2)
            relay_y(3)
            landed(e_in.at[3], er_sem.at[3])
            get_rows(0, 4)
            need_odd(0)
            second(0, FIRST)
            need_odd(1)
            second(1, FIRST)
            take(far_rel, 1, 2)
            take(far_rel, 0, 2)
            hand_on(own_rel, 0, 3)
            weigh(3, False)
            need_odd(2)
            second(2, FIRST)
            third(0, FIRST)
            third(1, FIRST)
            take_pair(2, 0)
            take_pair(2, 1)
            need(2, 0)
            need(2, 1)
            first(0, FIRST)
            take(far_rel, 1, 3)
            take(far_rel, 0, 3)
            need_odd(3)
            second(3, FIRST)
            third(2, FIRST)
            third(3, FIRST)
            get_rows(4, 6)
            first(0, SECOND_A)
            second(0, SECOND_A)
            second(1, SECOND_A)
            get_rows(6, 8)
            first(0, SECOND_B)
            second(0, SECOND_B)
            second(1, SECOND_B)
            second(2, SECOND)
            second(3, SECOND)
            for h in (2, 3):
                take_pair(2, h)
                need(2, h)
            first(1, FIRST)
            first(1, SECOND)

        @pl.when(source_even & (own_rel == 2))
        def _():
            hand_on(own_rel, 0, 1)
            landed(w_in, w_sem.at[1])
            weigh(0)
            relay_y(0)
            weigh(1)
            relay_y(1)
            hand_on(own_rel, 0, 2)
            relay_y(2)
            weigh(2)
            relay_y(3)
            hand_on(own_rel, 0, 3)
            weigh(3)
            get_rows(0, 4)
            for two in range(2):
                need(2, 2 * two)
                need(2, 2 * two + 1)
                first(two, FIRST)
            get_rows(4, 6)
            first(0, SECOND_A)
            take_odd(0)
            for h in range(2):
                take_pair(far_rel, h)

        @pl.when(source_even & (own_rel == 0))
        def _():
            hand_on(own_rel, 0, 1)
            hand_on(own_rel, 0, 2)
            landed(w_in, w_sem.at[1])
            relay_y(0)
            take_pair(far_rel, 0)
            relay_y(1)
            weigh(0)
            take_pair(far_rel, 1)
            relay_y(2)
            relay_y(3)
            for h in range(1, PIECES):
                landed(e_in.at[h], er_sem.at[h])
            get_rows(0, 4)
            need(2, 0)
            need(2, 1)
            first(0, FIRST)
            take_pair(far_rel, 2)
            need(2, 2)
            first_one(2, FIRST)
            weigh(1, False)
            get_rows(4, 6)
            first(0, SECOND_A)
            take_odd(0)
            take_pair(far_rel, 3)
            need(2, 3)
            first_one(3, FIRST)
            hand_on(own_rel, 0, 3)
            for h in (2, 3):
                weigh(h, False)

        @pl.when(source_even)
        def _():
            need_odd(0)
            second(0, FIRST)
            second(0, SECOND_A)

            @pl.when(own_rel == 2)
            def _():
                for h in (2, 3):
                    take_pair(far_rel, h)

            get_rows(6, 8)
            first(0, SECOND_B)
            second(0, SECOND_B)
            first(1, SECOND)
            take_odd(1)
            need_odd(1)
            second(1, FIRST)
            second(1, SECOND_A)
            second(1, SECOND_B)
            third(0, FIRST)
            third(1, FIRST)
            third(0, SECOND_A)
            third(1, SECOND_A)
            get_rows(8, 12)
            first(0, THIRD)
            first(1, THIRD)
            take_odd(2)
            need_odd(2)
            second(2, FIRST)
            second(2, SECOND)

    def begin_bridge():
        for h in range(2):
            to_source(h).start()
        for h in range(PIECES):
            for side in range(2):
                to_via_y(side, h).start()
        w_copy().start()
        send_rows(0, 2)
        for h in range(2, PIECES):
            to_source(h).start()
        load_others.wait()
        for i in range(4):
            span = pl.ds(i * SUB, SUB)
            high, low = split(e_ref[span, :])
            e_hi[span, :depth] = high
            e_lo[span, :depth] = low
        relay_x(1)
        send_rows(2, 6)
        relay_x(3)
        send_rows(6, 16)
        odd_next = lax.rem(odd_rel + 2, 4)
        take_pair(odd_rel, 0)
        take_pair(2, 0)
        take_pair(odd_next, 0)
        landed(w_in, w_sem.at[1])
        for i in range(4):
            landed(e_in.at[i], er_sem.at[i])
        get_rows(0, 4)
        need_odd(0)
        second(0, FIRST)
        need(2, 0)
        first_one(0, FIRST)
        take_pair(2, 1)
        need(2, 1)
        first_one(1, FIRST)
        take_pair(odd_rel, 1)
        take_pair(odd_next, 1)
        need_odd(1)
        second(1, FIRST)
        get_rows(4, 6)
        first(0, SECOND_A)
        second(0, SECOND_A)
        second(1, SECOND_A)
        take_pair(2, 2)
        third(0, FIRST)
        third(1, FIRST)
        need(2, 2)
        first_one(2, FIRST)
        take_pair(2, 3)
        need(2, 3)
        first_one(3, FIRST)
    def get_rows(start, stop):
        for i in range(start, stop):
            if start > 0:
                landed(e_in.at[i], er_sem.at[i])
            span = pl.ds(i * PROWS, PROWS)
            high, low = split(e_in[i])
            e_hi[span, depth:] = high
            e_lo[span, depth:] = low

    def dot(a, b):
        return lax.dot_general(a, b, (((1,), (1,)), ((), ())), preferred_element_type=F32)

    def ring(way):
        return (lax.rem(z + 1 + 2 * way, 4) * 2 + xl, r)

    def first_copy(way, h, chunk):
        slots = pl.ds(*chunk)
        return copy(
            part.at[h // 2, slots, pl.ds((h % 2) * 2 * PROWS + way * PROWS, PROWS)],
            first_in.at[way, h, slots],
            zs_sem, first_sem.at[way, h, SLOTS.index(chunk[0])], ring(way),
        )

    def second_copy(way, h, chunk):
        slots = pl.ds(*chunk)
        return copy(
            part.at[2 + h, slots, pl.ds((1 + way) * PROWS, PROWS)], second_in.at[way, h, slots],
            zs_sem, later_sem.at[0, way, h, SLOTS.index(chunk[0])], ring(way),
        )

    def third_copy(way, h, chunk):
        slots = pl.ds(*chunk)
        return copy(
            part.at[2 + h, slots, pl.ds(3 * way * PROWS, PROWS)], third_in.at[way, h, slots],
            zs_sem, later_sem.at[1, way, h, SLOTS.index(chunk[0])], ring(way),
        )

    here = z >= 0

    def product(block, chunk, top=0, count=SUB):
        span = pl.ds(pl.multiple_of(chunk[0] * WIDE, WIDE), chunk[1] * WIDE)
        rows_of = pl.ds(top, count)
        total = dot(p_hi[block, rows_of], e_hi[span, :])
        total += dot(p_hi[block, rows_of], e_lo[span, :])
        total += dot(p_lo[block, rows_of], e_hi[span, :])
        for i in range(chunk[1]):
            part[block, chunk[0] + i, rows_of] = total[:, i * WIDE : (i + 1) * WIDE]

    def first(two, chunk):
        pl.when(here)(lambda: product(two, chunk))
        for h in (2 * two, 2 * two + 1):
            for way in range(2):
                first_copy(way, h, chunk).start()

    def first_one(h, chunk):
        pl.when(here)(lambda: product(h // 2, chunk, (h % 2) * 2 * PROWS, 2 * PROWS))
        for way in range(2):
            first_copy(way, h, chunk).start()

    def second(h, chunk):
        pl.when(here)(lambda: product(2 + h, chunk))
        for way in range(2):
            second_copy(way, h, chunk).start()

    def second_all(chunk):
        def step(h, carry):
            product(2 + h, chunk)
            for way in range(2):
                second_copy(way, h, chunk).start()
            return carry

        lax.fori_loop(0, PIECES, step, 0)

    def third(h, chunk):
        slots = pl.ds(*chunk)
        for way in range(2):
            landed(first_in.at[way, h, slots], first_sem.at[way, h, SLOTS.index(chunk[0])])
            for i in range(chunk[0], chunk[0] + chunk[1]):
                part[2 + h, i, 3 * way * PROWS : (3 * way + 1) * PROWS] += first_in[way, h, i]
            third_copy(way, h, chunk).start()

    def last_parts():
        def step(n, carry):
            product(6 + n // 4, (lax.rem(n, 4) * 2, 2))
            return carry

        lax.fori_loop(0, 8, step, 0)

    def finish(h, chunk):
        slots = pl.ds(*chunk)
        for k in range(2):
            landed(second_in.at[1 - k, h, slots], later_sem.at[0, 1 - k, h, SLOTS.index(chunk[0])])
            landed(third_in.at[k, h, slots], later_sem.at[1, k, h, SLOTS.index(chunk[0])])
            piece = pl.ds(pl.multiple_of(h * PROWS, PROWS), PROWS)
            rows_of = pl.ds(pl.multiple_of(k * SUB + h * PROWS, PROWS), PROWS)
            for i in range(chunk[0], chunk[0] + chunk[1]):
                total = part[6 + k, i, piece] + (third_in[k, h, i] + second_in[1 - k, h, i])
                out_ref[rows_of, i * WIDE : (i + 1) * WIDE] = total

    def begin():
        pl.when(source)(begin_source)
        pl.when(bridge)(begin_bridge)

    def more(h):
        @pl.when(bridge if h == 2 else not_odd)
        def _():
            take_odd(h)
            need_odd(h)
            second(h, FIRST)
            second(h, SECOND)

    def pass_own():
        @pl.when(bridge)
        def _():
            for h in range(PIECES):
                take_pair(0, h)

    def own_parts():
        @pl.when(source_odd)
        def _():
            for h in range(PIECES):
                take_pair(0, h)

        for h in range(PIECES):
            need(0, h)

    def middle():
        @pl.when(bridge)
        def _():
            get_rows(6, 8)
            first(0, SECOND_B)
            second(0, SECOND_B)
            first(1, SECOND)
            second(1, SECOND_B)

    def now_third():
        @pl.when(jnp.logical_not(source_even))
        def _():
            third(0, SECOND_A)
            third(1, SECOND_A)

    def now_first():
        @pl.when(jnp.logical_not(source_even))
        def _():
            get_rows(8, 12)
            first(0, THIRD)
            first(1, THIRD)

    def middle_third():
        @pl.when(not_odd)
        def _():
            third(2, FIRST)
            third(3, FIRST)

    begin()
    middle()
    more(2)
    now_third()
    third(0, SECOND_B)
    third(1, SECOND_B)
    now_first()
    more(3)
    pass_own()
    middle_third()
    third(2, SECOND)
    third(3, SECOND)
    second_all(THIRD)
    get_rows(12, 16)
    first(0, FOURTH)
    first(1, FOURTH)
    third(0, THIRD)
    third(1, THIRD)
    second(0, FOURTH)
    third(2, THIRD)
    second(1, FOURTH)
    third(3, THIRD)
    second(2, FOURTH)
    second(3, FOURTH)
    own_parts()
    last_parts()
    for h in range(PIECES):
        third(h, FOURTH)
    def finish_all(start, stop, chunks):
        def step(h, carry):
            for chunk in chunks:
                finish(h, chunk)
            return carry

        lax.fori_loop(start, stop, step, 0)

    finish_all(0, 2, (FIRST, SECOND_A, SECOND_B))
    finish_all(2, 4, (FIRST, SECOND))
    finish_all(0, 4, (THIRD,))
    finish_all(0, 4, (FOURTH,))

    w_copy().wait_send()
    landed(e_ref, es_sem)
    landed(p_buf.at[pl.ds(0, 2)], cs_sem)
    landed(p_buf.at[pl.ds(0, 3)], zs_sem)

    @pl.when(source)
    def _():
        landed(p_buf.at[pl.ds(0, 3), 0, 0], xs_sem)
        landed(p_buf.at[pl.ds(0, 3), 0], ys_sem)

    @pl.when(bridge)
    def _():
        landed(p_buf.at[pl.ds(0, 3), 0, 0], xs_sem)
        landed(via_x, xs_sem)
        landed(p_buf.at[0], ys_sem)


def shards(eigvecs, slice_counts, occ_index, occ_levels):
    rows, depth = eigvecs.shape
    dma = pltpu.SemaphoreType.DMA
    levels = occ_levels.shape[0]
    slots = rows // WIDE
    return pl.pallas_call(
        kernel,
        out_shape=pltpu.VMEM((2 * SUB, rows), F32),
        in_specs=[pl.BlockSpec(memory_space=pl.ANY)] * 4,
        out_specs=pl.BlockSpec(memory_space=pltpu.VMEM),
        scratch_shapes=[
            pltpu.VMEM((rows, depth), F32),
            pltpu.VMEM((1, depth), jnp.int32),
            pltpu.VMEM((1, levels), F32),
            pltpu.VMEM((1, 1), jnp.int32),
            dma((5,)),
            pltpu.VMEM((4, 2, 2, PIECES, PROWS, depth), F32),
            pltpu.VMEM((PIECES, PROWS, depth), F32),
            pltpu.VMEM((2, PROWS, depth), F32),
            pltpu.VMEM((2, PIECES, PROWS, depth), F32),
            pltpu.VMEM((8, depth), F32),
            pltpu.VMEM((8, depth), F32),
            pltpu.VMEM((rows // PROWS, PROWS, depth), F32),
            pltpu.VMEM((8, SUB, 2 * depth), BF16),
            pltpu.VMEM((8, SUB, 2 * depth), BF16),
            pltpu.VMEM((rows, 2 * depth), BF16),
            pltpu.VMEM((rows, 2 * depth), BF16),
            pltpu.VMEM((8, slots, SUB, WIDE), F32),
            pltpu.VMEM((2, PIECES, slots, PROWS, WIDE), F32),
            pltpu.VMEM((2, PIECES, slots, PROWS, WIDE), F32),
            pltpu.VMEM((2, PIECES, slots, PROWS, WIDE), F32),
            dma((2,)),
            dma((2,)),
            dma((2, PIECES)),
            dma,
            dma,
            dma,
            dma((4, 2, 2, PIECES)),
            dma,
            dma((rows // PROWS,)),
            dma,
            dma((2, PIECES, len(SLOTS))),
            dma((2, 2, PIECES, len(SLOTS))),
        ],
        compiler_params=pltpu.CompilerParams(
            collective_id=0, has_side_effects=True, vmem_limit_bytes=60 * 1024 * 1024
        ),
    )(
        eigvecs,
        occ_index.reshape(1, depth),
        occ_levels.reshape(1, levels),
        slice_counts.reshape(1, 1),
    )


def solution(mesh):
    return jax.shard_map(
        shards,
        mesh=mesh,
        in_specs=(P("row", "cuts"), P("cuts"), P("cuts"), P()),
        out_specs=P("cuts", "row"),
        check_vma=False,
    )
```

```python
import jax
import jax.numpy as jnp
from jax import lax
from jax.experimental import pallas as pl
from jax.experimental.pallas import tpu as pltpu
from jax.sharding import PartitionSpec as P

MESH = pl.DeviceIdType.MESH
SUB = 256
PIECES = 4
PROWS = SUB // PIECES
WIDE = 128
FIRST, SECOND, THIRD, FOURTH = (0, 2), (2, 2), (4, 2), (6, 2)
SECOND_A, SECOND_B = (2, 1), (3, 1)
SLOTS = (0, 2, 3, 4, 6)
F32, BF16 = jnp.float32, jnp.bfloat16


def split(value):
    high = value.astype(BF16)
    return high, (value - high.astype(F32)).astype(BF16)


def kernel(
    e_any, idx_any, lev_any, cnt_any, out_any,
    out_ref, out_sem, e_ref, idx_ref, lev_ref, cnt_ref, in_sem, p_buf, own_p, via_x, via_y, w_own, w_in, e_in, p_hi, p_lo, e_hi, e_lo, part, first_in, second_in, third_in,
    w_sem, vx_sem, vy_sem, xs_sem, ys_sem, cs_sem, p_sem, es_sem, er_sem, zs_sem, first_sem, later_sem,
):
    rows, depth = e_ref.shape
    c, r = lax.axis_index("cuts"), lax.axis_index("row")
    z, xl = c // 2, lax.rem(c, 2)
    q, core = r // 2, lax.rem(r, 2)
    xh, y = q // 4, lax.rem(q, 4)
    x = xh * 2 + xl

    def device(dx=0, dy=0, dz=0, dcore=0):
        nx, ny = lax.rem(x + dx + 4, 4), lax.rem(y + dy + 4, 4)
        nz, ncore = lax.rem(z + dz + 4, 4), lax.rem(core + dcore, 2)
        return (nz * 2 + lax.rem(nx, 2), ((nx // 2) * 4 + ny) * 2 + ncore)

    pair = (z * 2 + 1 - xl, r)
    other = device(dx=3 - 2 * xl)
    source = lax.rem(y, 2) == xl
    even_row = y // 2 == lax.rem(z, 2)
    bridge = jnp.logical_not(source)
    source_odd = source & jnp.logical_not(even_row)

    source_even = source & even_row
    not_odd = jnp.logical_not(source_odd)

    def base(dy):
        return lax.rem(2 * xh + lax.rem(y + dy, 4) // 2 - z + 4, 4)

    own_rel = base(0)
    far_rel = lax.rem(own_rel + 2, 4)

    def row_gap(rel):
        return lax.rem(2 * lax.rem(z + rel, 2) + xl - y + 4, 4)

    barrier = pltpu.get_barrier_semaphore()
    for peer in (
        device(dx=1), device(dx=2), device(dx=3), device(dy=1), device(dy=3),
        device(dz=1), device(dz=3), device(dcore=1),
    ):
        pl.semaphore_signal(barrier, inc=1, device_id=peer, device_id_type=MESH)

    picked, others = pl.ds(0, SUB), pl.ds(SUB, rows - SUB)
    small = [
        pltpu.make_async_copy(src, dst, in_sem.at[n])
        for n, (src, dst) in enumerate(
            ((idx_any, idx_ref), (lev_any, lev_ref), (cnt_any, cnt_ref))
        )
    ]
    load_picked = pltpu.make_async_copy(e_any.at[picked], e_ref.at[picked], in_sem.at[3])
    load_others = pltpu.make_async_copy(e_any.at[others], e_ref.at[others], in_sem.at[4])
    for load in (*small, load_picked, load_others):
        load.start()
    for load in small:
        load.wait()
    count = lev_ref.shape[1]
    diagonal = lax.broadcasted_iota(jnp.int32, (count, count), 0) == lax.broadcasted_iota(
        jnp.int32, (count, count), 1
    )
    levels = jnp.sum(jnp.where(diagonal, lev_ref[...], F32(0.0)), axis=1, keepdims=True)
    level = lax.broadcasted_iota(jnp.int32, (count, depth), 0)
    chosen = jnp.where(level == idx_ref[...], levels, F32(0.0))
    values = jnp.sum(chosen, axis=0, keepdims=True)
    live = lax.broadcasted_iota(jnp.int32, (1, depth), 1) < cnt_ref[...]
    weights = jnp.where(live, values, F32(0.0))
    w_own[...] = jnp.broadcast_to(weights, w_own.shape)
    load_picked.wait()
    for h in range(PIECES):
        own_p[h] = e_ref[h * PROWS : (h + 1) * PROWS, :] * weights

    @pl.when(source)
    def _():
        for h in range(PIECES):
            p_buf[own_rel, core, 0, h] = own_p[h]

    pl.semaphore_wait(barrier, 8)

    def copy(src, dst, send, recv, peer):
        return pltpu.make_async_remote_copy(
            src_ref=src, dst_ref=dst, send_sem=send, recv_sem=recv,
            device_id=peer, device_id_type=MESH,
        )

    def w_copy():
        return copy(w_own, w_in, w_sem.at[0], w_sem.at[1], pair)

    def e_copy(i):
        return copy(e_ref.at[pl.ds(i * PROWS, PROWS)], e_in.at[i], es_sem, er_sem.at[i], pair)

    def slot_of(rel, s, h):
        return p_buf.at[rel, core, s, h], p_sem.at[rel, core, s, h]

    def to_twin(h):
        slot, recv = slot_of(own_rel, 0, h)
        return copy(own_p.at[h], slot, xs_sem, recv, device(dx=2))

    def to_via_x(h):
        return copy(own_p.at[h], via_x.at[h // 2], xs_sem, vx_sem.at[h // 2], other)

    def from_via_x(h):
        slot, recv = slot_of(far_rel, 0, h)
        return copy(via_x.at[h // 2], slot, xs_sem, recv, pair)

    def to_source(h):
        slot, recv = slot_of(own_rel, 1, h)
        return copy(own_p.at[h], slot, xs_sem, recv, other)

    def to_via_y(side, h):
        return copy(
            own_p.at[h], via_y.at[side, h], xs_sem, vy_sem.at[side, h],
            device(dy=3 if side == 0 else 1),
        )

    def from_via_y(side, h):
        slot, recv = slot_of(base(1 if side == 0 else 3), 1, h)
        return copy(via_y.at[side, h], slot, xs_sem, recv, other)

    def y_copy(rel, s, h, up):
        slot, recv = slot_of(rel, s, h)
        return copy(slot, slot, ys_sem, recv, device(dy=1 if up else 3))

    def core_copy(rel, s, h):
        slot, recv = slot_of(rel, s, h)
        return copy(slot, slot, cs_sem, recv, device(dcore=1))

    def landed(ref, sem):
        pltpu.make_async_copy(ref, ref, sem).wait()

    def arrive(rel, k, s, h):
        landed(p_buf.at[rel, k, s, h], p_sem.at[rel, k, s, h])

    def spot(rel, k, h):
        odd = lax.rem(rel, 2)
        block = jnp.where(odd == 1, 2 + h, jnp.where(rel == 2, h // 2, 6 + k))
        row = jnp.where(
            odd == 1,
            (rel // 2) * 2 * PROWS + k * PROWS,
            jnp.where(rel == 2, lax.rem(h, 2) * 2 * PROWS + k * PROWS, h * PROWS),
        )
        return block, pl.ds(pl.multiple_of(row, PROWS), PROWS)

    def keep(rel, k, s, h):
        high, low = split(p_buf[rel, k, s, h])
        block, rows_of = spot(rel, k, h)
        p_hi[block, rows_of, s * depth : (s + 1) * depth] = high
        p_lo[block, rows_of, s * depth : (s + 1) * depth] = low

    def sends(rel, s, up):
        gap = row_gap(rel)
        first_hop = gap == 0
        if s == 1:
            first_hop = first_hop & (rel != far_rel)
        if up and s == 0:
            return first_hop | (gap == 3)
        if not up and s == 1:
            return first_hop | (gap == 1)
        return first_hop

    def hand_on(rel, s, h):
        for up in (True, False):
            pl.when(sends(rel, s, up))(lambda up=up: y_copy(rel, s, h, up).start())
        core_copy(rel, s, h).start()
        keep(rel, core, s, h)

    def take(rel, s, h):
        arrive(rel, core, s, h)
        hand_on(rel, s, h)

    def weigh(h, wait=True):
        if wait:
            landed(e_in.at[h], er_sem.at[h])
        p_buf[own_rel, core, 1, h] = e_in[h] * w_in[0:1, :]
        hand_on(own_rel, 1, h)

    def need(rel, h):
        for s in range(2):
            arrive(rel, 1 - core, s, h)
            keep(rel, 1 - core, s, h)

    def need_odd(h):
        need(1, h)
        need(3, h)

    def relay_x(h):
        landed(via_x.at[h // 2], vx_sem.at[h // 2])
        from_via_x(h).start()

    def relay_y(h):
        for side in range(2):
            landed(via_y.at[side, h], vy_sem.at[side, h])
            from_via_y(side, h).start()

    def send_rows(start, stop):
        for i in range(start, stop):
            e_copy(i).start()

    def take_pair(rel, h):
        take(rel, 0, h)
        take(rel, 1, h)

    odd_rel = jnp.where(lax.rem(base(1), 2) == 1, base(1), base(3))
    odd_rel = jnp.where(source, base(2), odd_rel)

    def take_odd(h):
        take_pair(odd_rel, h)
        take_pair(lax.rem(odd_rel + 2, 4), h)

    def send_others():
        load_others.wait()
        send_rows(4, 16)
        for i in range(4):
            span = pl.ds(i * SUB, SUB)
            high, low = split(e_ref[span, :])
            e_hi[span, :depth] = high
            e_lo[span, :depth] = low

    def begin_source():
        to_twin(0).start()
        to_via_x(1).start()
        to_via_x(3).start()
        w_copy().start()
        send_rows(0, 4)
        to_twin(2).start()
        hand_on(own_rel, 0, 0)
        send_others()

        @pl.when(source_odd)
        def _():
            hand_on(own_rel, 0, 1)
            landed(w_in, w_sem.at[1])
            weigh(0)
            relay_y(0)
            take(far_rel, 1, 0)
            take(far_rel, 0, 0)
            weigh(1)
            relay_y(1)
            take(far_rel, 1, 1)
            take(far_rel, 0, 1)
            relay_y(2)
            hand_on(own_rel, 0, 2)
            weigh(2)
            relay_y(3)
            landed(e_in.at[3], er_sem.at[3])
            get_rows(0, 4)
            need_odd(0)
            second(0, FIRST)
            need_odd(1)
            second(1, FIRST)
            take(far_rel, 1, 2)
            take(far_rel, 0, 2)
            hand_on(own_rel, 0, 3)
            weigh(3, False)
            need_odd(2)
            second(2, FIRST)
            third(0, FIRST)
            third(1, FIRST)
            take_pair(2, 0)
            take_pair(2, 1)
            need(2, 0)
            need(2, 1)
            first(0, FIRST)
            take(far_rel, 1, 3)
            take(far_rel, 0, 3)
            need_odd(3)
            second(3, FIRST)
            third(2, FIRST)
            third(3, FIRST)
            get_rows(4, 6)
            first(0, SECOND_A)
            second(0, SECOND_A)
            second(1, SECOND_A)
            get_rows(6, 8)
            first(0, SECOND_B)
            second(0, SECOND_B)
            second(1, SECOND_B)
            second(2, SECOND)
            second(3, SECOND)
            for h in (2, 3):
                take_pair(2, h)
                need(2, h)
            first(1, FIRST)
            first(1, SECOND)

        @pl.when(source_even & (own_rel == 2))
        def _():
            hand_on(own_rel, 0, 1)
            landed(w_in, w_sem.at[1])
            weigh(0)
            relay_y(0)
            weigh(1)
            relay_y(1)
            hand_on(own_rel, 0, 2)
            relay_y(2)
            weigh(2)
            relay_y(3)
            hand_on(own_rel, 0, 3)
            weigh(3)
            get_rows(0, 4)
            for two in range(2):
                need(2, 2 * two)
                need(2, 2 * two + 1)
                first(two, FIRST)
            get_rows(4, 6)
            first(0, SECOND_A)
            take_odd(0)
            for h in range(2):
                take_pair(far_rel, h)

        @pl.when(source_even & (own_rel == 0))
        def _():
            hand_on(own_rel, 0, 1)
            hand_on(own_rel, 0, 2)
            landed(w_in, w_sem.at[1])
            relay_y(0)
            take_pair(far_rel, 0)
            relay_y(1)
            weigh(0)
            take_pair(far_rel, 1)
            relay_y(2)
            relay_y(3)
            for h in range(1, PIECES):
                landed(e_in.at[h], er_sem.at[h])
            get_rows(0, 4)
            need(2, 0)
            need(2, 1)
            first(0, FIRST)
            take_pair(far_rel, 2)
            need(2, 2)
            first_one(2, FIRST)
            weigh(1, False)
            get_rows(4, 6)
            first(0, SECOND_A)
            take_odd(0)
            take_pair(far_rel, 3)
            need(2, 3)
            first_one(3, FIRST)
            hand_on(own_rel, 0, 3)
            for h in (2, 3):
                weigh(h, False)

        @pl.when(source_even)
        def _():
            need_odd(0)
            second(0, FIRST)
            second(0, SECOND_A)

            @pl.when(own_rel == 2)
            def _():
                for h in (2, 3):
                    take_pair(far_rel, h)

            get_rows(6, 8)
            first(0, SECOND_B)
            second(0, SECOND_B)
            first(1, SECOND)
            take_odd(1)
            need_odd(1)
            second(1, FIRST)
            second(1, SECOND_A)
            second(1, SECOND_B)
            third(0, FIRST)
            third(1, FIRST)
            third(0, SECOND_A)
            third(1, SECOND_A)
            get_rows(8, 12)
            first(0, THIRD)
            first(1, THIRD)
            take_odd(2)
            need_odd(2)
            second(2, FIRST)
            second(2, SECOND)

    def begin_bridge():
        for h in range(2):
            to_source(h).start()
        for h in range(PIECES):
            for side in range(2):
                to_via_y(side, h).start()
        w_copy().start()
        send_rows(0, 2)
        for h in range(2, PIECES):
            to_source(h).start()
        load_others.wait()
        for i in range(4):
            span = pl.ds(i * SUB, SUB)
            high, low = split(e_ref[span, :])
            e_hi[span, :depth] = high
            e_lo[span, :depth] = low
        relay_x(1)
        send_rows(2, 6)
        relay_x(3)
        send_rows(6, 16)
        odd_next = lax.rem(odd_rel + 2, 4)
        take_pair(odd_rel, 0)
        take_pair(2, 0)
        take_pair(odd_next, 0)
        landed(w_in, w_sem.at[1])
        for i in range(4):
            landed(e_in.at[i], er_sem.at[i])
        get_rows(0, 4)
        need_odd(0)
        second(0, FIRST)
        need(2, 0)
        first_one(0, FIRST)
        take_pair(2, 1)
        need(2, 1)
        first_one(1, FIRST)
        take_pair(odd_rel, 1)
        take_pair(odd_next, 1)
        need_odd(1)
        second(1, FIRST)
        get_rows(4, 6)
        first(0, SECOND_A)
        second(0, SECOND_A)
        second(1, SECOND_A)
        take_pair(2, 2)
        third(0, FIRST)
        third(1, FIRST)
        need(2, 2)
        first_one(2, FIRST)
        take_pair(2, 3)
        need(2, 3)
        first_one(3, FIRST)
    def get_rows(start, stop):
        for i in range(start, stop):
            if start > 0:
                landed(e_in.at[i], er_sem.at[i])
            span = pl.ds(i * PROWS, PROWS)
            high, low = split(e_in[i])
            e_hi[span, depth:] = high
            e_lo[span, depth:] = low

    def dot(a, b):
        return lax.dot_general(a, b, (((1,), (1,)), ((), ())), preferred_element_type=F32)

    def ring(way):
        return (lax.rem(z + 1 + 2 * way, 4) * 2 + xl, r)

    def first_copy(way, h, chunk):
        slots = pl.ds(*chunk)
        return copy(
            part.at[h // 2, slots, pl.ds((h % 2) * 2 * PROWS + way * PROWS, PROWS)],
            first_in.at[way, h, slots],
            zs_sem, first_sem.at[h, SLOTS.index(chunk[0])], ring(way),
        )

    def second_copy(way, h, chunk):
        slots = pl.ds(*chunk)
        return copy(
            part.at[2 + h, slots, pl.ds((1 + way) * PROWS, PROWS)], second_in.at[way, h, slots],
            zs_sem, later_sem.at[0, h, SLOTS.index(chunk[0])], ring(way),
        )

    def third_copy(way, h, chunk):
        slots = pl.ds(*chunk)
        return copy(
            part.at[2 + h, slots, pl.ds(3 * way * PROWS, PROWS)], third_in.at[way, h, slots],
            zs_sem, later_sem.at[1, h, SLOTS.index(chunk[0])], ring(way),
        )

    here = z >= 0

    def product(block, chunk, top=0, count=SUB):
        span = pl.ds(pl.multiple_of(chunk[0] * WIDE, WIDE), chunk[1] * WIDE)
        rows_of = pl.ds(top, count)
        total = dot(p_hi[block, rows_of], e_hi[span, :])
        total += dot(p_hi[block, rows_of], e_lo[span, :])
        total += dot(p_lo[block, rows_of], e_hi[span, :])
        for i in range(chunk[1]):
            part[block, chunk[0] + i, rows_of] = total[:, i * WIDE : (i + 1) * WIDE]

    def first(two, chunk):
        pl.when(here)(lambda: product(two, chunk))
        for h in (2 * two, 2 * two + 1):
            for way in range(2):
                first_copy(way, h, chunk).start()

    def first_one(h, chunk):
        pl.when(here)(lambda: product(h // 2, chunk, (h % 2) * 2 * PROWS, 2 * PROWS))
        for way in range(2):
            first_copy(way, h, chunk).start()

    def second(h, chunk):
        pl.when(here)(lambda: product(2 + h, chunk))
        for way in range(2):
            second_copy(way, h, chunk).start()

    def second_all(chunk):
        def step(h, carry):
            product(2 + h, chunk)
            for way in range(2):
                second_copy(way, h, chunk).start()
            return carry

        lax.fori_loop(0, PIECES, step, 0)

    def third(h, chunk):
        slots = pl.ds(*chunk)
        landed(first_in.at[:, h, slots], first_sem.at[h, SLOTS.index(chunk[0])])
        for way in range(2):
            for i in range(chunk[0], chunk[0] + chunk[1]):
                part[2 + h, i, 3 * way * PROWS : (3 * way + 1) * PROWS] += first_in[way, h, i]
            third_copy(way, h, chunk).start()

    def last_parts():
        def step(n, carry):
            product(6 + n // 4, (lax.rem(n, 4) * 2, 2))
            return carry

        lax.fori_loop(0, 8, step, 0)

    def finish(h, chunk):
        slots = pl.ds(*chunk)
        landed(second_in.at[:, h, slots], later_sem.at[0, h, SLOTS.index(chunk[0])])
        landed(third_in.at[:, h, slots], later_sem.at[1, h, SLOTS.index(chunk[0])])
        for k in range(2):
            piece = pl.ds(pl.multiple_of(h * PROWS, PROWS), PROWS)
            rows_of = pl.ds(pl.multiple_of(k * SUB + h * PROWS, PROWS), PROWS)
            for i in range(chunk[0], chunk[0] + chunk[1]):
                total = part[6 + k, i, piece] + (third_in[k, h, i] + second_in[1 - k, h, i])
                out_ref[rows_of, i * WIDE : (i + 1) * WIDE] = total

    def begin():
        pl.when(source)(begin_source)
        pl.when(bridge)(begin_bridge)

    def more(h):
        @pl.when(bridge if h == 2 else not_odd)
        def _():
            take_odd(h)
            need_odd(h)
            second(h, FIRST)
            second(h, SECOND)

    def pass_own():
        @pl.when(bridge)
        def _():
            for h in range(PIECES):
                take_pair(0, h)

    def own_parts():
        @pl.when(source_odd)
        def _():
            for h in range(PIECES):
                take_pair(0, h)

        for h in range(PIECES):
            need(0, h)

    def middle():
        @pl.when(bridge)
        def _():
            get_rows(6, 8)
            first(0, SECOND_B)
            second(0, SECOND_B)
            first(1, SECOND)
            second(1, SECOND_B)

    def now_third():
        @pl.when(jnp.logical_not(source_even))
        def _():
            third(0, SECOND_A)
            third(1, SECOND_A)

    def now_first():
        @pl.when(jnp.logical_not(source_even))
        def _():
            get_rows(8, 12)
            first(0, THIRD)
            first(1, THIRD)

    def middle_third():
        @pl.when(not_odd)
        def _():
            third(2, FIRST)
            third(3, FIRST)

    begin()
    middle()
    more(2)
    now_third()
    third(0, SECOND_B)
    third(1, SECOND_B)
    now_first()
    more(3)
    pass_own()
    middle_third()
    third(2, SECOND)
    third(3, SECOND)
    second_all(THIRD)
    get_rows(12, 16)
    first(0, FOURTH)
    first(1, FOURTH)
    third(0, THIRD)
    third(1, THIRD)
    second(0, FOURTH)
    third(2, THIRD)
    second(1, FOURTH)
    third(3, THIRD)
    second(2, FOURTH)
    second(3, FOURTH)
    own_parts()
    last_parts()
    for h in range(PIECES):
        third(h, FOURTH)
    def finish_all(start, stop, chunks):
        def step(h, carry):
            for chunk in chunks:
                finish(h, chunk)
            return carry

        lax.fori_loop(start, stop, step, 0)

    def put(rows_of, columns):
        pltpu.make_async_copy(
            out_ref.at[rows_of, columns], out_any.at[rows_of, columns], out_sem
        ).start()

    finish_all(0, 2, (FIRST, SECOND_A, SECOND_B))
    finish_all(2, 4, (FIRST, SECOND))
    put(pl.ds(0, 2 * SUB), pl.ds(0, 4 * WIDE))
    finish_all(0, 4, (THIRD,))
    put(pl.ds(0, 2 * SUB), pl.ds(4 * WIDE, 2 * WIDE))
    for h in range(PIECES):
        finish(h, FOURTH)
        for k in range(2):
            put(pl.ds(k * SUB + h * PROWS, PROWS), pl.ds(6 * WIDE, 2 * WIDE))

    pltpu.make_async_copy(out_ref, out_any, out_sem).wait()
    w_copy().wait_send()
    landed(e_ref, es_sem)
    landed(p_buf.at[pl.ds(0, 2)], cs_sem)
    landed(p_buf.at[pl.ds(0, 3)], zs_sem)

    @pl.when(source)
    def _():
        landed(p_buf.at[pl.ds(0, 3), 0, 0], xs_sem)
        landed(p_buf.at[pl.ds(0, 3), 0], ys_sem)

    @pl.when(bridge)
    def _():
        landed(p_buf.at[pl.ds(0, 3), 0, 0], xs_sem)
        landed(via_x, xs_sem)
        landed(p_buf.at[0], ys_sem)


def shards(eigvecs, slice_counts, occ_index, occ_levels):
    rows, depth = eigvecs.shape
    dma = pltpu.SemaphoreType.DMA
    levels = occ_levels.shape[0]
    slots = rows // WIDE
    return pl.pallas_call(
        kernel,
        out_shape=pltpu.VMEM((2 * SUB, rows), F32),
        in_specs=[pl.BlockSpec(memory_space=pl.ANY)] * 4,
        out_specs=pl.BlockSpec(memory_space=pl.ANY),
        scratch_shapes=[
            pltpu.VMEM((2 * SUB, rows), F32),
            dma,
            pltpu.VMEM((rows, depth), F32),
            pltpu.VMEM((1, depth), jnp.int32),
            pltpu.VMEM((1, levels), F32),
            pltpu.VMEM((1, 1), jnp.int32),
            dma((5,)),
            pltpu.VMEM((4, 2, 2, PIECES, PROWS, depth), F32),
            pltpu.VMEM((PIECES, PROWS, depth), F32),
            pltpu.VMEM((2, PROWS, depth), F32),
            pltpu.VMEM((2, PIECES, PROWS, depth), F32),
            pltpu.VMEM((8, depth), F32),
            pltpu.VMEM((8, depth), F32),
            pltpu.VMEM((rows // PROWS, PROWS, depth), F32),
            pltpu.VMEM((8, SUB, 2 * depth), BF16),
            pltpu.VMEM((8, SUB, 2 * depth), BF16),
            pltpu.VMEM((rows, 2 * depth), BF16),
            pltpu.VMEM((rows, 2 * depth), BF16),
            pltpu.VMEM((8, slots, SUB, WIDE), F32),
            pltpu.VMEM((2, PIECES, slots, PROWS, WIDE), F32),
            pltpu.VMEM((2, PIECES, slots, PROWS, WIDE), F32),
            pltpu.VMEM((2, PIECES, slots, PROWS, WIDE), F32),
            dma((2,)),
            dma((2,)),
            dma((2, PIECES)),
            dma,
            dma,
            dma,
            dma((4, 2, 2, PIECES)),
            dma,
            dma((rows // PROWS,)),
            dma,
            dma((PIECES, len(SLOTS))),
            dma((2, PIECES, len(SLOTS))),
        ],
        compiler_params=pltpu.CompilerParams(
            collective_id=0, has_side_effects=True, vmem_limit_bytes=60 * 1024 * 1024
        ),
    )(
        eigvecs,
        occ_index.reshape(1, depth),
        occ_levels.reshape(1, levels),
        slice_counts.reshape(1, 1),
    )


def solution(mesh):
    return jax.shard_map(
        shards,
        mesh=mesh,
        in_specs=(P("row", "cuts"), P("cuts"), P("cuts"), P()),
        out_specs=P("cuts", "row"),
        check_vma=False,
    )
```

```python
import jax
import jax.numpy as jnp
from jax import lax
from jax.experimental import pallas as pl
from jax.experimental.pallas import tpu as pltpu
from jax.sharding import PartitionSpec as P

MESH = pl.DeviceIdType.MESH
SUB = 256
PIECES = 4
PROWS = SUB // PIECES
WIDE = 128
FIRST, SECOND, THIRD, FOURTH = (0, 2), (2, 2), (4, 2), (6, 2)
SECOND_A, SECOND_B = (2, 1), (3, 1)
SLOTS = (0, 2, 3, 4, 6)
F32, BF16 = jnp.float32, jnp.bfloat16


def split(value):
    high = value.astype(BF16)
    return high, (value - high.astype(F32)).astype(BF16)


def kernel(
    e_any, idx_any, lev_any, cnt_any, out_any,
    out_ref, out_sem, e_ref, idx_ref, lev_ref, cnt_ref, in_sem, p_buf, own_p, via_x, via_y, w_own, w_in, e_in, p_hi, p_lo, e_hi, e_lo, part, first_in, second_in, third_in,
    w_sem, vx_sem, vy_sem, xs_sem, ys_sem, cs_sem, p_sem, es_sem, er_sem, zs_sem, first_sem, later_sem,
):
    rows, depth = e_ref.shape
    c, r = lax.axis_index("cuts"), lax.axis_index("row")
    z, xl = c // 2, lax.rem(c, 2)
    q, core = r // 2, lax.rem(r, 2)
    xh, y = q // 4, lax.rem(q, 4)
    x = xh * 2 + xl

    def device(dx=0, dy=0, dz=0, dcore=0):
        nx, ny = lax.rem(x + dx + 4, 4), lax.rem(y + dy + 4, 4)
        nz, ncore = lax.rem(z + dz + 4, 4), lax.rem(core + dcore, 2)
        return (nz * 2 + lax.rem(nx, 2), ((nx // 2) * 4 + ny) * 2 + ncore)

    pair = (z * 2 + 1 - xl, r)
    other = device(dx=3 - 2 * xl)
    source = lax.rem(y, 2) == xl
    even_row = y // 2 == lax.rem(z, 2)
    bridge = jnp.logical_not(source)
    source_odd = source & jnp.logical_not(even_row)

    source_even = source & even_row
    not_odd = jnp.logical_not(source_odd)

    def base(dy):
        return lax.rem(2 * xh + lax.rem(y + dy, 4) // 2 - z + 4, 4)

    own_rel = base(0)
    far_rel = lax.rem(own_rel + 2, 4)

    def row_gap(rel):
        return lax.rem(2 * lax.rem(z + rel, 2) + xl - y + 4, 4)

    barrier = pltpu.get_barrier_semaphore()
    for peer in (
        device(dx=1), device(dx=2), device(dx=3), device(dy=1), device(dy=3),
        device(dz=1), device(dz=3), device(dcore=1),
    ):
        pl.semaphore_signal(barrier, inc=1, device_id=peer, device_id_type=MESH)

    picked, others = pl.ds(0, SUB), pl.ds(SUB, rows - SUB)
    small = [
        pltpu.make_async_copy(src, dst, in_sem.at[n])
        for n, (src, dst) in enumerate(
            ((idx_any, idx_ref), (lev_any, lev_ref), (cnt_any, cnt_ref))
        )
    ]
    load_picked = pltpu.make_async_copy(e_any.at[picked], e_ref.at[picked], in_sem.at[3])
    load_others = pltpu.make_async_copy(e_any.at[others], e_ref.at[others], in_sem.at[4])
    for load in (*small, load_picked, load_others):
        load.start()
    for load in small:
        load.wait()
    count = lev_ref.shape[1]
    diagonal = lax.broadcasted_iota(jnp.int32, (count, count), 0) == lax.broadcasted_iota(
        jnp.int32, (count, count), 1
    )
    levels = jnp.sum(jnp.where(diagonal, lev_ref[...], F32(0.0)), axis=1, keepdims=True)
    level = lax.broadcasted_iota(jnp.int32, (count, depth), 0)
    chosen = jnp.where(level == idx_ref[...], levels, F32(0.0))
    values = jnp.sum(chosen, axis=0, keepdims=True)
    live = lax.broadcasted_iota(jnp.int32, (1, depth), 1) < cnt_ref[...]
    weights = jnp.where(live, values, F32(0.0))
    w_own[...] = jnp.broadcast_to(weights, w_own.shape)
    load_picked.wait()
    for h in range(PIECES):
        own_p[h] = e_ref[h * PROWS : (h + 1) * PROWS, :] * weights

    @pl.when(source)
    def _():
        for h in range(PIECES):
            p_buf[own_rel, core, 0, h] = own_p[h]

    pl.semaphore_wait(barrier, 8)

    def copy(src, dst, send, recv, peer):
        return pltpu.make_async_remote_copy(
            src_ref=src, dst_ref=dst, send_sem=send, recv_sem=recv,
            device_id=peer, device_id_type=MESH,
        )

    def w_copy():
        return copy(w_own, w_in, w_sem.at[0], w_sem.at[1], pair)

    def e_copy(i):
        return copy(e_ref.at[pl.ds(i * PROWS, PROWS)], e_in.at[i], es_sem, er_sem.at[i], pair)

    def slot_of(rel, s, h):
        return p_buf.at[rel, core, s, h], p_sem.at[rel, core, s, h]

    def to_twin(h):
        slot, recv = slot_of(own_rel, 0, h)
        return copy(own_p.at[h], slot, xs_sem, recv, device(dx=2))

    def to_via_x(h):
        return copy(own_p.at[h], via_x.at[h // 2], xs_sem, vx_sem.at[h // 2], other)

    def from_via_x(h):
        slot, recv = slot_of(far_rel, 0, h)
        return copy(via_x.at[h // 2], slot, xs_sem, recv, pair)

    def to_source(h):
        slot, recv = slot_of(own_rel, 1, h)
        return copy(own_p.at[h], slot, xs_sem, recv, other)

    def to_via_y(side, h):
        return copy(
            own_p.at[h], via_y.at[side, h], xs_sem, vy_sem.at[side, h],
            device(dy=3 if side == 0 else 1),
        )

    def from_via_y(side, h):
        slot, recv = slot_of(base(1 if side == 0 else 3), 1, h)
        return copy(via_y.at[side, h], slot, xs_sem, recv, other)

    def y_copy(rel, s, h, up):
        slot, recv = slot_of(rel, s, h)
        return copy(slot, slot, ys_sem, recv, device(dy=1 if up else 3))

    def core_copy(rel, s, h):
        slot, recv = slot_of(rel, s, h)
        return copy(slot, slot, cs_sem, recv, device(dcore=1))

    def landed(ref, sem):
        pltpu.make_async_copy(ref, ref, sem).wait()

    def arrive(rel, k, s, h):
        landed(p_buf.at[rel, k, s, h], p_sem.at[rel, k, s, h])

    def spot(rel, k, h):
        odd = lax.rem(rel, 2)
        block = jnp.where(odd == 1, 2 + h, jnp.where(rel == 2, h // 2, 6 + k))
        row = jnp.where(
            odd == 1,
            (rel // 2) * 2 * PROWS + k * PROWS,
            jnp.where(rel == 2, lax.rem(h, 2) * 2 * PROWS + k * PROWS, h * PROWS),
        )
        return block, pl.ds(pl.multiple_of(row, PROWS), PROWS)

    def keep(rel, k, s, h):
        high, low = split(p_buf[rel, k, s, h])
        block, rows_of = spot(rel, k, h)
        p_hi[block, rows_of, s * depth : (s + 1) * depth] = high
        p_lo[block, rows_of, s * depth : (s + 1) * depth] = low

    def sends(rel, s, up):
        gap = row_gap(rel)
        first_hop = gap == 0
        if s == 1:
            first_hop = first_hop & (rel != far_rel)
        if up and s == 0:
            return first_hop | (gap == 3)
        if not up and s == 1:
            return first_hop | (gap == 1)
        return first_hop

    def hand_on(rel, s, h):
        for up in (True, False):
            pl.when(sends(rel, s, up))(lambda up=up: y_copy(rel, s, h, up).start())
        core_copy(rel, s, h).start()
        keep(rel, core, s, h)

    def take(rel, s, h):
        arrive(rel, core, s, h)
        hand_on(rel, s, h)

    def weigh(h, wait=True):
        if wait:
            landed(e_in.at[h], er_sem.at[h])
        p_buf[own_rel, core, 1, h] = e_in[h] * w_in[0:1, :]
        hand_on(own_rel, 1, h)

    def need(rel, h):
        for s in range(2):
            arrive(rel, 1 - core, s, h)
            keep(rel, 1 - core, s, h)

    def need_odd(h):
        need(1, h)
        need(3, h)

    def relay_x(h):
        landed(via_x.at[h // 2], vx_sem.at[h // 2])
        from_via_x(h).start()

    def relay_y(h):
        for side in range(2):
            landed(via_y.at[side, h], vy_sem.at[side, h])
            from_via_y(side, h).start()

    def send_rows(start, stop):
        for i in range(start, stop):
            e_copy(i).start()

    def take_pair(rel, h):
        take(rel, 0, h)
        take(rel, 1, h)

    odd_rel = jnp.where(lax.rem(base(1), 2) == 1, base(1), base(3))
    odd_rel = jnp.where(source, base(2), odd_rel)

    def take_odd(h):
        take_pair(odd_rel, h)
        take_pair(lax.rem(odd_rel + 2, 4), h)

    def send_others():
        load_others.wait()
        send_rows(4, 16)
        for i in range(4):
            span = pl.ds(i * SUB, SUB)
            high, low = split(e_ref[span, :])
            e_hi[span, :depth] = high
            e_lo[span, :depth] = low

    def begin_source():
        to_twin(0).start()
        to_via_x(1).start()
        to_via_x(3).start()
        w_copy().start()
        send_rows(0, 4)
        to_twin(2).start()
        hand_on(own_rel, 0, 0)
        send_others()

        @pl.when(source_odd)
        def _():
            hand_on(own_rel, 0, 1)
            landed(w_in, w_sem.at[1])
            weigh(0)
            relay_y(0)
            take(far_rel, 0, 0)
            take(far_rel, 1, 0)
            weigh(1)
            relay_y(1)
            take(far_rel, 0, 1)
            take(far_rel, 1, 1)
            relay_y(2)
            hand_on(own_rel, 0, 2)
            weigh(2)
            relay_y(3)
            landed(e_in.at[3], er_sem.at[3])
            get_rows(0, 4)
            need_odd(0)
            second(0, FIRST)
            need_odd(1)
            second(1, FIRST)
            take(far_rel, 0, 2)
            take(far_rel, 1, 2)
            hand_on(own_rel, 0, 3)
            weigh(3, False)
            need_odd(2)
            second(2, FIRST)
            third(0, FIRST)
            third(1, FIRST)
            take_pair(2, 0)
            take_pair(2, 1)
            need(2, 0)
            need(2, 1)
            first(0, FIRST)
            take(far_rel, 0, 3)
            take(far_rel, 1, 3)
            need_odd(3)
            second(3, FIRST)
            third(2, FIRST)
            third(3, FIRST)
            get_rows(4, 6)
            first(0, SECOND_A)
            second(0, SECOND_A)
            second(1, SECOND_A)
            get_rows(6, 8)
            first(0, SECOND_B)
            second(0, SECOND_B)
            second(1, SECOND_B)
            second(2, SECOND)
            second(3, SECOND)
            for h in (2, 3):
                take_pair(2, h)
                need(2, h)
            first(1, FIRST)
            first(1, SECOND)

        @pl.when(source_even & (own_rel == 2))
        def _():
            hand_on(own_rel, 0, 1)
            landed(w_in, w_sem.at[1])
            weigh(0)
            relay_y(0)
            weigh(1)
            relay_y(1)
            hand_on(own_rel, 0, 2)
            relay_y(2)
            weigh(2)
            relay_y(3)
            hand_on(own_rel, 0, 3)
            weigh(3)
            get_rows(0, 4)
            for two in range(2):
                need(2, 2 * two)
                need(2, 2 * two + 1)
                first(two, FIRST)
            get_rows(4, 6)
            first(0, SECOND_A)
            take_odd(0)
            for h in range(2):
                take_pair(far_rel, h)

        @pl.when(source_even & (own_rel == 0))
        def _():
            hand_on(own_rel, 0, 1)
            hand_on(own_rel, 0, 2)
            landed(w_in, w_sem.at[1])
            relay_y(0)
            take_pair(far_rel, 0)
            relay_y(1)
            weigh(0)
            take_pair(far_rel, 1)
            relay_y(2)
            relay_y(3)
            for h in range(1, PIECES):
                landed(e_in.at[h], er_sem.at[h])
            get_rows(0, 4)
            need(2, 0)
            need(2, 1)
            first(0, FIRST)
            take_pair(far_rel, 2)
            need(2, 2)
            first_one(2, FIRST)
            weigh(1, False)
            get_rows(4, 6)
            first(0, SECOND_A)
            take_odd(0)
            take_pair(far_rel, 3)
            need(2, 3)
            first_one(3, FIRST)
            hand_on(own_rel, 0, 3)
            for h in (2, 3):
                weigh(h, False)

        @pl.when(source_even)
        def _():
            need_odd(0)
            second(0, FIRST)
            second(0, SECOND_A)

            @pl.when(own_rel == 2)
            def _():
                for h in (2, 3):
                    take_pair(far_rel, h)

            get_rows(6, 8)
            first(0, SECOND_B)
            second(0, SECOND_B)
            first(1, SECOND)
            take_odd(1)
            need_odd(1)
            second(1, FIRST)
            second(1, SECOND_A)
            second(1, SECOND_B)
            third(0, FIRST)
            third(1, FIRST)
            third(0, SECOND_A)
            third(1, SECOND_A)
            get_rows(8, 12)
            first(0, THIRD)
            first(1, THIRD)
            take_odd(2)
            need_odd(2)
            second(2, FIRST)
            second(2, SECOND)

    def begin_bridge():
        for h in range(2):
            to_source(h).start()
        for h in range(PIECES):
            for side in range(2):
                to_via_y(side, h).start()
        w_copy().start()
        send_rows(0, 2)
        for h in range(2, PIECES):
            to_source(h).start()
        load_others.wait()
        for i in range(4):
            span = pl.ds(i * SUB, SUB)
            high, low = split(e_ref[span, :])
            e_hi[span, :depth] = high
            e_lo[span, :depth] = low
        relay_x(1)
        send_rows(2, 6)
        relay_x(3)
        send_rows(6, 16)
        odd_next = lax.rem(odd_rel + 2, 4)
        take_pair(odd_rel, 0)
        take_pair(2, 0)
        take_pair(odd_next, 0)
        landed(w_in, w_sem.at[1])
        for i in range(4):
            landed(e_in.at[i], er_sem.at[i])
        get_rows(0, 4)
        need_odd(0)
        second(0, FIRST)
        need(2, 0)
        first_one(0, FIRST)
        take_pair(2, 1)
        need(2, 1)
        first_one(1, FIRST)
        take_pair(odd_rel, 1)
        take_pair(odd_next, 1)
        need_odd(1)
        second(1, FIRST)
        get_rows(4, 6)
        first(0, SECOND_A)
        second(0, SECOND_A)
        second(1, SECOND_A)
        take_pair(2, 2)
        third(0, FIRST)
        third(1, FIRST)
        need(2, 2)
        first_one(2, FIRST)
        take_pair(2, 3)
        need(2, 3)
        first_one(3, FIRST)
    def get_rows(start, stop):
        for i in range(start, stop):
            if start > 0:
                landed(e_in.at[i], er_sem.at[i])
            span = pl.ds(i * PROWS, PROWS)
            high, low = split(e_in[i])
            e_hi[span, depth:] = high
            e_lo[span, depth:] = low

    def dot(a, b):
        return lax.dot_general(a, b, (((1,), (1,)), ((), ())), preferred_element_type=F32)

    def ring(way):
        return (lax.rem(z + 1 + 2 * way, 4) * 2 + xl, r)

    def first_copy(way, h, chunk):
        slots = pl.ds(*chunk)
        return copy(
            part.at[h // 2, slots, pl.ds((h % 2) * 2 * PROWS + way * PROWS, PROWS)],
            first_in.at[way, h, slots],
            zs_sem, first_sem.at[h, SLOTS.index(chunk[0])], ring(way),
        )

    def second_copy(way, h, chunk):
        slots = pl.ds(*chunk)
        return copy(
            part.at[2 + h, slots, pl.ds((1 + way) * PROWS, PROWS)], second_in.at[way, h, slots],
            zs_sem, later_sem.at[0, h, SLOTS.index(chunk[0])], ring(way),
        )

    def third_copy(way, h, chunk):
        slots = pl.ds(*chunk)
        return copy(
            part.at[2 + h, slots, pl.ds(3 * way * PROWS, PROWS)], third_in.at[way, h, slots],
            zs_sem, later_sem.at[1, h, SLOTS.index(chunk[0])], ring(way),
        )

    here = z >= 0

    def product(block, chunk, top=0, count=SUB):
        span = pl.ds(pl.multiple_of(chunk[0] * WIDE, WIDE), chunk[1] * WIDE)
        rows_of = pl.ds(top, count)
        total = dot(p_hi[block, rows_of], e_hi[span, :])
        total += dot(p_hi[block, rows_of], e_lo[span, :])
        total += dot(p_lo[block, rows_of], e_hi[span, :])
        for i in range(chunk[1]):
            part[block, chunk[0] + i, rows_of] = total[:, i * WIDE : (i + 1) * WIDE]

    def first(two, chunk):
        pl.when(here)(lambda: product(two, chunk))
        for h in (2 * two, 2 * two + 1):
            for way in range(2):
                first_copy(way, h, chunk).start()

    def first_one(h, chunk):
        pl.when(here)(lambda: product(h // 2, chunk, (h % 2) * 2 * PROWS, 2 * PROWS))
        for way in range(2):
            first_copy(way, h, chunk).start()

    def second(h, chunk):
        pl.when(here)(lambda: product(2 + h, chunk))
        for way in range(2):
            second_copy(way, h, chunk).start()

    def second_all(chunk):
        def step(h, carry):
            product(2 + h, chunk)
            for way in range(2):
                second_copy(way, h, chunk).start()
            return carry

        lax.fori_loop(0, PIECES, step, 0)

    def third(h, chunk):
        slots = pl.ds(*chunk)
        landed(first_in.at[:, h, slots], first_sem.at[h, SLOTS.index(chunk[0])])
        for way in range(2):
            for i in range(chunk[0], chunk[0] + chunk[1]):
                part[2 + h, i, 3 * way * PROWS : (3 * way + 1) * PROWS] += first_in[way, h, i]
            third_copy(way, h, chunk).start()

    def last_parts():
        def step(n, carry):
            product(6 + n // 4, (lax.rem(n, 4) * 2, 2))
            return carry

        lax.fori_loop(0, 8, step, 0)

    def finish(h, chunk):
        slots = pl.ds(*chunk)
        landed(second_in.at[:, h, slots], later_sem.at[0, h, SLOTS.index(chunk[0])])
        landed(third_in.at[:, h, slots], later_sem.at[1, h, SLOTS.index(chunk[0])])
        for k in range(2):
            piece = pl.ds(pl.multiple_of(h * PROWS, PROWS), PROWS)
            rows_of = pl.ds(pl.multiple_of(k * SUB + h * PROWS, PROWS), PROWS)
            for i in range(chunk[0], chunk[0] + chunk[1]):
                total = part[6 + k, i, piece] + (third_in[k, h, i] + second_in[1 - k, h, i])
                out_ref[rows_of, i * WIDE : (i + 1) * WIDE] = total

    def begin():
        pl.when(source)(begin_source)
        pl.when(bridge)(begin_bridge)

    def more(h):
        @pl.when(bridge if h == 2 else not_odd)
        def _():
            take_odd(h)
            need_odd(h)
            second(h, FIRST)
            second(h, SECOND)

    def pass_own():
        @pl.when(bridge)
        def _():
            for h in range(PIECES):
                take_pair(0, h)

    def own_parts():
        @pl.when(source_odd)
        def _():
            for h in range(PIECES):
                take_pair(0, h)

        for h in range(PIECES):
            need(0, h)

    def middle():
        @pl.when(bridge)
        def _():
            get_rows(6, 8)
            first(0, SECOND_B)
            second(0, SECOND_B)
            first(1, SECOND)
            second(1, SECOND_B)

    def now_third():
        @pl.when(jnp.logical_not(source_even))
        def _():
            third(0, SECOND_A)
            third(1, SECOND_A)

    def now_first():
        @pl.when(jnp.logical_not(source_even))
        def _():
            get_rows(8, 12)
            first(0, THIRD)
            first(1, THIRD)

    def middle_third():
        @pl.when(not_odd)
        def _():
            third(2, FIRST)
            third(3, FIRST)

    begin()
    middle()
    more(2)
    now_third()
    third(0, SECOND_B)
    third(1, SECOND_B)
    now_first()
    more(3)
    pass_own()
    middle_third()
    third(2, SECOND)
    third(3, SECOND)
    second_all(THIRD)
    get_rows(12, 16)
    first(0, FOURTH)
    first(1, FOURTH)
    third(0, THIRD)
    third(1, THIRD)
    second(0, FOURTH)
    third(2, THIRD)
    second(1, FOURTH)
    third(3, THIRD)
    second(2, FOURTH)
    second(3, FOURTH)
    own_parts()
    last_parts()
    for h in range(PIECES):
        third(h, FOURTH)
    def finish_all(start, stop, chunks):
        def step(h, carry):
            for chunk in chunks:
                finish(h, chunk)
            return carry

        lax.fori_loop(start, stop, step, 0)

    def put(rows_of, columns):
        pltpu.make_async_copy(
            out_ref.at[rows_of, columns], out_any.at[rows_of, columns], out_sem
        ).start()

    finish_all(0, 2, (FIRST, SECOND_A, SECOND_B))
    finish_all(2, 4, (FIRST, SECOND))
    put(pl.ds(0, 2 * SUB), pl.ds(0, 4 * WIDE))
    finish_all(0, 4, (THIRD,))
    put(pl.ds(0, 2 * SUB), pl.ds(4 * WIDE, 2 * WIDE))
    for h in range(PIECES):
        finish(h, FOURTH)
        for k in range(2):
            put(pl.ds(k * SUB + h * PROWS, PROWS), pl.ds(6 * WIDE, 2 * WIDE))

    pltpu.make_async_copy(out_ref, out_any, out_sem).wait()
    w_copy().wait_send()
    landed(e_ref, es_sem)
    landed(p_buf.at[pl.ds(0, 2)], cs_sem)
    landed(p_buf.at[pl.ds(0, 3)], zs_sem)

    @pl.when(source)
    def _():
        landed(p_buf.at[pl.ds(0, 3), 0, 0], xs_sem)
        landed(p_buf.at[pl.ds(0, 3), 0], ys_sem)

    @pl.when(bridge)
    def _():
        landed(p_buf.at[pl.ds(0, 3), 0, 0], xs_sem)
        landed(via_x, xs_sem)
        landed(p_buf.at[0], ys_sem)


def shards(eigvecs, slice_counts, occ_index, occ_levels):
    rows, depth = eigvecs.shape
    dma = pltpu.SemaphoreType.DMA
    levels = occ_levels.shape[0]
    slots = rows // WIDE
    return pl.pallas_call(
        kernel,
        out_shape=pltpu.VMEM((2 * SUB, rows), F32),
        in_specs=[pl.BlockSpec(memory_space=pl.ANY)] * 4,
        out_specs=pl.BlockSpec(memory_space=pl.ANY),
        scratch_shapes=[
            pltpu.VMEM((2 * SUB, rows), F32),
            dma,
            pltpu.VMEM((rows, depth), F32),
            pltpu.VMEM((1, depth), jnp.int32),
            pltpu.VMEM((1, levels), F32),
            pltpu.VMEM((1, 1), jnp.int32),
            dma((5,)),
            pltpu.VMEM((4, 2, 2, PIECES, PROWS, depth), F32),
            pltpu.VMEM((PIECES, PROWS, depth), F32),
            pltpu.VMEM((2, PROWS, depth), F32),
            pltpu.VMEM((2, PIECES, PROWS, depth), F32),
            pltpu.VMEM((8, depth), F32),
            pltpu.VMEM((8, depth), F32),
            pltpu.VMEM((rows // PROWS, PROWS, depth), F32),
            pltpu.VMEM((8, SUB, 2 * depth), BF16),
            pltpu.VMEM((8, SUB, 2 * depth), BF16),
            pltpu.VMEM((rows, 2 * depth), BF16),
            pltpu.VMEM((rows, 2 * depth), BF16),
            pltpu.VMEM((8, slots, SUB, WIDE), F32),
            pltpu.VMEM((2, PIECES, slots, PROWS, WIDE), F32),
            pltpu.VMEM((2, PIECES, slots, PROWS, WIDE), F32),
            pltpu.VMEM((2, PIECES, slots, PROWS, WIDE), F32),
            dma((2,)),
            dma((2,)),
            dma((2, PIECES)),
            dma,
            dma,
            dma,
            dma((4, 2, 2, PIECES)),
            dma,
            dma((rows // PROWS,)),
            dma,
            dma((PIECES, len(SLOTS))),
            dma((2, PIECES, len(SLOTS))),
        ],
        compiler_params=pltpu.CompilerParams(
            collective_id=0, has_side_effects=True, vmem_limit_bytes=60 * 1024 * 1024
        ),
    )(
        eigvecs,
        occ_index.reshape(1, depth),
        occ_levels.reshape(1, levels),
        slice_counts.reshape(1, 1),
    )


def solution(mesh):
    return jax.shard_map(
        shards,
        mesh=mesh,
        in_specs=(P("row", "cuts"), P("cuts"), P("cuts"), P()),
        out_specs=P("cuts", "row"),
        check_vma=False,
    )
```
